16 devices in a mesh: depth: 2 (over z), col: 2 (over y), row: 4 (over x, core).
Axes of the slice: x: 2, y: 2, z: 2, core: 2. Of those that a mesh axis runs over, the one named last changes fastest.
Arguments:
- weight: bfloat16 [2048, 2048], P(('row', 'depth'), 'col')
- rhs_stack: bfloat16 [3, 2048, 8192], P(None, ('row', 'depth'), 'col')
Outputs:
- output: bfloat16 [3, 2048, 8192], P(None, ('row', 'depth'), 'col')
All inputs are finite; a program needn't handle non-finite values.
Results may differ from the reference program's by a relative error of at most 0.001.
Values are sent between devices in bfloat16 or wider.
A program may use at most 1 GiB of HBM per device.

```python
import jax
import jax.numpy as jnp
from jax import lax

N = 2048
RHS_COLS = 8192


def setup_inputs(seed: int = 0) -> dict:
    base_key = jax.random.key(seed)
    key_w, key_x = jax.random.split(base_key)
    weight = jax.random.normal(key_w, (N, N), jnp.float32) * (N ** -0.5) + 2.0 / N
    rhs_stack = jax.random.normal(key_x, (3, N, RHS_COLS), jnp.float32) + 0.5
    return {"weight": weight.astype(jnp.bfloat16), "rhs_stack": rhs_stack.astype(jnp.bfloat16)}


def reference(weight, rhs_stack):
    def one_product(rhs_block):
        return jnp.dot(weight, rhs_block, preferred_element_type=jnp.float32).astype(jnp.bfloat16)
    return lax.map(one_product, rhs_stack)
```

```python
import jax
import jax.numpy as jnp
from jax import lax
from jax.sharding import PartitionSpec as P


def solution(mesh):
    plane = ("row", "depth")

    def local(w, x):
        w = lax.all_gather(w, "col", axis=1, tiled=True)
        w = lax.all_gather(w, plane, axis=0, tiled=True)
        xs = lax.all_to_all(x, plane, split_axis=2, concat_axis=1, tiled=True)
        y = jnp.einsum("mk,rkn->rmn", w, xs, preferred_element_type=jnp.float32).astype(jnp.bfloat16)
        return lax.all_to_all(y, plane, split_axis=1, concat_axis=2, tiled=True)

    return jax.shard_map(local, mesh=mesh, in_specs=(P(("row", "depth"), "col"), P(None, ("row", "depth"), "col")),
                         out_specs=P(None, ("row", "depth"), "col"), check_vma=False)
```

```python
import functools

import jax
import jax.numpy as jnp
from jax import lax
from jax.experimental import pallas as pl
from jax.experimental.pallas import tpu as pltpu
from jax.sharding import PartitionSpec as P

MESH = pl.DeviceIdType.MESH
PEERS = 8
HALVES = 2
PIECE = 256


def kernel(w_ref, x_ref, y_ref, a_buf, x_buf, y_buf, a_send, a_recv, x_send, x_recv, y_send, y_recv, own_sem):
    z, j, row = lax.axis_index("depth"), lax.axis_index("col"), lax.axis_index("row")
    x, c = row // 2, row % 2
    rhs, rows, _ = x_ref.shape
    kcols = w_ref.shape[1]
    chunks = rhs * HALVES

    def place(px, pc, pz):
        return (px * 2 + pc) * 2 + pz

    def peer(k):
        kx, kc, kz = k // 4 % 2, k // 2 % 2, k % 2
        px = x + kx * (1 - 2 * x)
        pc = c + kc * (1 - 2 * c)
        pz = z + kz * (1 - 2 * z)
        return (pz, j, px * 2 + pc), place(px, pc, pz)

    me = place(x, c, z)

    def a_block(g, jj):
        return a_buf.at[pl.ds(pl.multiple_of(g * rows, rows), rows), pl.ds(pl.multiple_of(jj * kcols, kcols), kcols)]

    fx, fz = x + (1 - c) * (1 - 2 * x), z + c * (1 - 2 * z)
    sx, sz = x + c * (1 - 2 * x), z + (1 - c) * (1 - 2 * z)
    first, second = (fz, j, fx * 2 + c), (sz, j, sx * 2 + c)
    other_y, other_core = (z, 1 - j, row), (z, j, x * 2 + 1 - c)
    spots = [(x, z), (fx, fz), (sx, sz), (1 - x, 1 - z)]
    mine = [place(px, c, pz) for px, pz in spots]
    theirs = [place(px, 1 - c, pz) for px, pz in (spots[0], spots[2], spots[1], spots[3])]

    def a_copy(n):
        if n == 0:
            src, here, there, to = w_ref, a_block(mine[1], j), a_block(me, j), first
        elif n == 1:
            src, here, there, to = w_ref, a_block(mine[2], j), a_block(me, j), second
        elif n == 2:
            src, here, there, to = a_block(mine[1], j), a_block(mine[3], j), a_block(mine[1], j), second
        elif n < 7:
            b = n - 3
            there = a_block(mine[b], j)
            src, here, to = (w_ref if b == 0 else there), a_block(mine[b], 1 - j), other_y
        elif n < 11:
            b = n - 7
            there = a_block(mine[b], j)
            src, here, to = (w_ref if b == 0 else there), a_block(theirs[b], j), other_core
        else:
            b = n - 11
            there = a_block(mine[b], 1 - j)
            src, here, to = there, a_block(theirs[b], 1 - j), other_core
        send = pltpu.make_async_remote_copy(src, there, a_send.at[n], a_recv.at[n], device_id=to, device_id_type=MESH)
        recv = pltpu.make_async_remote_copy(src, here, a_send.at[n], a_recv.at[n], device_id=to, device_id_type=MESH)
        return send, recv

    def a_start(n):
        a_copy(n)[0].start()

    def a_wait(n):
        a_copy(n)[1].wait_recv()

    def x_cols(chunk, g):
        return x_ref.at[chunk // HALVES, :, pl.ds(pl.multiple_of(g * (HALVES * PIECE) + chunk % HALVES * PIECE, PIECE), PIECE)]

    def x_rows(chunk, g):
        return x_buf.at[chunk, pl.ds(pl.multiple_of(g * rows, rows), rows), :]

    def x_copy(chunk, k, receive=False):
        dev, g = peer(k)
        return pltpu.make_async_remote_copy(
            x_cols(chunk, g), x_rows(chunk, g if receive else me), x_send.at[chunk, k], x_recv.at[chunk, k],
            device_id=dev, device_id_type=MESH)

    def y_rows(chunk, g):
        return y_buf.at[chunk, pl.ds(pl.multiple_of(g * rows, rows), rows), :]

    def y_cols(chunk, g):
        return y_ref.at[chunk // HALVES, :, pl.ds(pl.multiple_of(g * (HALVES * PIECE) + chunk % HALVES * PIECE, PIECE), PIECE)]

    def y_copy(chunk, k, receive=False):
        dev, g = peer(k)
        return pltpu.make_async_remote_copy(
            y_rows(chunk, g), y_cols(chunk, g if receive else me), y_send.at[chunk, k], y_recv.at[chunk, k],
            device_id=dev, device_id_type=MESH)

    def own_x(chunk):
        return pltpu.make_async_copy(x_cols(chunk, me), x_rows(chunk, me), own_sem.at[chunk])

    def own_y(chunk):
        return pltpu.make_async_copy(y_rows(chunk, me), y_cols(chunk, me), own_sem.at[chunks + 1 + chunk])

    own_a = pltpu.make_async_copy(w_ref, a_block(me, j), own_sem.at[chunks])

    def send_x(chunk):
        own_x(chunk).start()
        for k in (5, 4, 1, 7, 6, 3, 2):
            x_copy(chunk, k).start()

    barrier = pltpu.get_barrier_semaphore()
    for k in range(1, PEERS):
        pl.semaphore_signal(barrier, inc=1, device_id=peer(k)[0], device_id_type=MESH)
    pl.semaphore_signal(barrier, inc=1, device_id=other_y, device_id_type=MESH)
    pl.semaphore_wait(barrier, PEERS)

    own_a.start()
    for n in (0, 1, 3, 7):
        a_start(n)
    send_x(0)
    a_wait(0)
    for n in (2, 4, 8):
        a_start(n)
    a_wait(1)
    for n in (5, 9):
        a_start(n)
    send_x(1)
    a_wait(2)
    for n in (6, 10):
        a_start(n)
    for chunk in range(2, chunks):
        send_x(chunk)
    for b in range(4):
        a_wait(3 + b)
        a_start(11 + b)
    for n in range(7, 15):
        a_wait(n)
    own_a.wait()

    def do_chunk(chunk, carry):
        own_x(chunk).wait()

        def arrive(k, carry):
            x_copy(chunk, k, receive=True).wait_recv()
            return carry

        lax.fori_loop(1, PEERS, arrive, 0)

        def tile(t, carry):
            k = (t + 1) % PEERS
            g = peer(k)[1]
            at = pl.ds(pl.multiple_of(g * rows, rows), rows)
            acc = jnp.dot(a_buf[at, :], x_buf[chunk], preferred_element_type=jnp.float32)
            y_buf[chunk, at, :] = acc.astype(y_buf.dtype)

            @pl.when(t > 0)
            def _():
                y_copy(chunk, t).start()

            return carry

        lax.fori_loop(0, PEERS, tile, 0)
        return carry

    lax.fori_loop(0, chunks, do_chunk, 0)

    for n in range(15):
        a_copy(n)[0].wait_send()

    def x_done(chunk, carry):
        def one(k, carry):
            x_copy(chunk, k).wait_send()
            return carry

        return lax.fori_loop(1, PEERS, one, carry)

    lax.fori_loop(0, chunks, x_done, 0)

    def own_out(chunk, carry):
        own_y(chunk).start()
        return carry

    lax.fori_loop(0, chunks, own_out, 0)

    def y_done(chunk, carry):
        def one(k, carry):
            y_copy(chunk, k).wait_send()
            y_copy(chunk, k, receive=True).wait_recv()
            return carry

        lax.fori_loop(1, PEERS, one, 0)
        own_y(chunk).wait()
        return carry

    lax.fori_loop(0, chunks, y_done, 0)


def solution(mesh):
    def local(w, x):
        rhs, rows, cols = x.shape
        n = rows * PEERS
        chunks = rhs * HALVES
        return pl.pallas_call(
            kernel,
            out_shape=jax.ShapeDtypeStruct(x.shape, x.dtype),
            in_specs=[pl.BlockSpec(memory_space=pl.ANY)] * 2,
            out_specs=pl.BlockSpec(memory_space=pl.ANY),
            scratch_shapes=[
                pltpu.VMEM((n, n), w.dtype),
                pltpu.VMEM((chunks, n, PIECE), x.dtype),
                pltpu.VMEM((chunks, n, PIECE), x.dtype),
                pltpu.SemaphoreType.DMA((15,)),
                pltpu.SemaphoreType.DMA((15,)),
                pltpu.SemaphoreType.DMA((chunks, PEERS)),
                pltpu.SemaphoreType.DMA((chunks, PEERS)),
                pltpu.SemaphoreType.DMA((chunks, PEERS)),
                pltpu.SemaphoreType.DMA((chunks, PEERS)),
                pltpu.SemaphoreType.DMA((2 * chunks + 1,)),
            ],
            compiler_params=pltpu.CompilerParams(collective_id=0, has_side_effects=True, vmem_limit_bytes=48 * 1024 * 1024),
        )(w, x)

    return jax.shard_map(local, mesh=mesh, in_specs=(P(("row", "depth"), "col"), P(None, ("row", "depth"), "col")),
                         out_specs=P(None, ("row", "depth"), "col"), check_vma=False)
```

```python
import jax
import jax.numpy as jnp
from jax import lax
from jax.experimental import pallas as pl
from jax.experimental.pallas import tpu as pltpu
from jax.sharding import PartitionSpec as P

MESH = pl.DeviceIdType.MESH
SIDE = 4
BLOCKS = 2 * SIDE
PIECE = 256
AHEAD = 3
LAG = 1


def kernel(w_ref, x_ref, y_ref, a_buf, x_buf, y_buf, a_send, a_recv, x_send, x_recv, y_send, y_recv, own_sem):
    z, j, row = lax.axis_index("depth"), lax.axis_index("col"), lax.axis_index("row")
    x, c = row // 2, row % 2
    rhs, rows, cols = x_ref.shape
    kcols = w_ref.shape[1]
    group = cols // SIDE
    pieces = group // PIECE
    steps = rhs * pieces

    def peer(k):
        kx, kc, kz = k // 4 % 2, k // 2 % 2, k % 2
        return x + kx * (1 - 2 * x), c + kc * (1 - 2 * c), z + kz * (1 - 2 * z)

    def device(k):
        px, pc, pz = peer(k)
        return (pz, j, px * 2 + pc)

    def in_side(k):
        _, pc, pz = peer(k)
        return pc * 2 + pz

    def in_plane(k):
        return peer(k)[0] * SIDE + in_side(k)

    other_y = (z, 1 - j, row)

    def a_block(k, jj):
        return a_buf.at[pl.ds(pl.multiple_of(in_side(k) * rows, rows), rows), pl.ds(pl.multiple_of(jj * kcols, kcols), kcols)]

    def a_copy(n, receive=False):
        own = (w_ref, a_block(0, j))
        src, there, here, to = (
            own + (a_block(1, j), device(1)),
            own + (a_block(0, 1 - j), other_y),
            (a_block(1, j),) * 2 + (a_block(1, 1 - j), other_y),
            own + (a_block(2, j), device(2)),
            (a_block(1, j),) * 2 + (a_block(3, j), device(2)),
            (a_block(0, 1 - j),) * 2 + (a_block(2, 1 - j), device(2)),
            (a_block(1, 1 - j),) * 2 + (a_block(3, 1 - j), device(2)),
        )[n]
        return pltpu.make_async_remote_copy(
            src, here if receive else there, a_send.at[n], a_recv.at[n], device_id=to, device_id_type=MESH)

    def columns(step, k):
        at = in_side(k) * group + step % pieces * PIECE
        return (step // pieces, slice(None), pl.ds(pl.multiple_of(at, PIECE), PIECE))

    def x_rows(step, k):
        return x_buf.at[step, pl.ds(pl.multiple_of(in_plane(k) * rows, rows), rows), :]

    def x_copy(step, k, receive=False):
        if k in (5, 7):
            src, there, to = x_rows(step, k - 4), x_rows(step, k - 4), device(4)
        else:
            src, there, to = x_ref.at[columns(step, k)], x_rows(step, 0), device(k)
        return pltpu.make_async_remote_copy(
            src, x_rows(step, k) if receive else there, x_send.at[step, k], x_recv.at[step, k],
            device_id=to, device_id_type=MESH)

    def y_rows(step, k):
        return y_buf.at[step, pl.ds(pl.multiple_of(in_side(k) * rows, rows), rows), :]

    def y_copy(step, k, receive=False):
        return pltpu.make_async_remote_copy(
            y_rows(step, k), y_ref.at[columns(step, k if receive else 0)], y_send.at[step, k], y_recv.at[step, k],
            device_id=device(k), device_id_type=MESH)

    def own_x(step):
        return pltpu.make_async_copy(x_ref.at[columns(step, 0)], x_rows(step, 0), own_sem.at[0, step])

    def own_y(step):
        return pltpu.make_async_copy(y_rows(step, 0), y_ref.at[columns(step, 0)], own_sem.at[1, step])

    own_a = pltpu.make_async_copy(w_ref, a_block(0, j), own_sem.at[2, 0])

    def send_x(step, ks):
        for k in ks:
            x_copy(step, k).start()

    def loop(low, high, body):
        def one(step, carry):
            body(step)
            return carry

        lax.fori_loop(low, high, one, 0)

    barrier = pltpu.get_barrier_semaphore()
    for to in [device(k) for k in (1, 2, 3, 4, 6)] + [other_y]:
        pl.semaphore_signal(barrier, inc=1, device_id=to, device_id_type=MESH)
    pl.semaphore_wait(barrier, 6)

    for n in (0, 1, 3):
        a_copy(n).start()
    own_a.start()

    def first(step):
        send_x(step, (1, 3))

        @pl.when(step < AHEAD)
        def _():
            send_x(step, (4, 6))

        send_x(step, (2,))
        own_x(step).start()

    loop(0, steps, first)

    a_copy(0, True).wait_recv()
    a_copy(2).start()
    a_copy(4).start()

    def forward(step):
        for k in (1, 3):
            x_copy(step, k, True).wait_recv()
            x_copy(step, k + 4).start()

        @pl.when(step + AHEAD < steps)
        def _():
            send_x(step + AHEAD, (4, 6))

    def multiply(step):
        own_x(step).wait()
        for k in (2, 4, 6, 5, 7):
            x_copy(step, k, True).wait_recv()
        for n, k in enumerate((1, 3, 2, 0)):
            at = pl.ds(pl.multiple_of(in_side(k) * rows, rows), rows)
            acc = jnp.dot(a_buf[at, :], x_buf[step], preferred_element_type=jnp.float32)
            y_buf[step, at, :] = acc.astype(y_buf.dtype)
            if n:
                y_copy(step, (1, 3, 2)[n - 1]).start()

    loop(0, LAG, forward)
    a_copy(1, True).wait_recv()
    a_copy(5).start()
    a_copy(2, True).wait_recv()
    a_copy(6).start()
    own_a.wait()
    for n in (3, 4, 5, 6):
        a_copy(n, True).wait_recv()

    def both(step):
        forward(step)
        multiply(step - LAG)

    loop(LAG, steps, both)
    loop(steps - LAG, steps, multiply)

    for n in range(7):
        a_copy(n).wait_send()

    def x_done(step):
        for k in range(1, BLOCKS):
            x_copy(step, k).wait_send()
        own_y(step).start()

    loop(0, steps, x_done)

    def y_done(step):
        for k in (1, 3, 2):
            y_copy(step, k).wait_send()
            y_copy(step, k, True).wait_recv()
        own_y(step).wait()

    loop(0, steps, y_done)


def solution(mesh):
    def local(w, x):
        rhs, rows, cols = x.shape
        n = rows * BLOCKS
        steps = rhs * (cols // SIDE // PIECE)
        sems = pltpu.SemaphoreType.DMA
        return pl.pallas_call(
            kernel,
            out_shape=pltpu.VMEM(x.shape, x.dtype),
            in_specs=[pl.BlockSpec(memory_space=pl.ANY)] * 2,
            out_specs=pl.BlockSpec(memory_space=pltpu.VMEM),
            scratch_shapes=[
                pltpu.VMEM((SIDE * rows, n), w.dtype),
                pltpu.VMEM((steps, n, PIECE), x.dtype),
                pltpu.VMEM((steps, SIDE * rows, PIECE), x.dtype),
                sems((7,)), sems((7,)),
                sems((steps, BLOCKS)), sems((steps, BLOCKS)),
                sems((steps, SIDE)), sems((steps, SIDE)),
                sems((3, steps)),
            ],
            compiler_params=pltpu.CompilerParams(collective_id=0, has_side_effects=True, vmem_limit_bytes=52 * 1024 * 1024),
        )(w, x)

    return jax.shard_map(local, mesh=mesh, in_specs=(P(("row", "depth"), "col"), P(None, ("row", "depth"), "col")),
                         out_specs=P(None, ("row", "depth"), "col"), check_vma=False)
```

```python
import jax
import jax.numpy as jnp
from jax import lax
from jax.experimental import pallas as pl
from jax.experimental.pallas import tpu as pltpu
from jax.sharding import PartitionSpec as P

MESH = pl.DeviceIdType.MESH
SIDE = 4
PIECES = ((0, 0, 512), (0, 512, 512), (1, 0, 512), (1, 512, 512), (2, 0, 512), (2, 512, 256), (2, 768, 256))
DIRECT = ((0, 0, 1024), (1, 0, 1024), (2, 0, 512), (2, 512, 512))
WIDE = 256


def kernel(w_ref, x_ref, y_ref, a_buf, x_buf, y_buf, a_send, a_recv, z_send, z_recv, d_send, d_recv, f_send, f_recv,
           p_send, p_recv, y_send, y_recv, q_send, q_recv, own_sem):
    z, j, row = lax.axis_index("depth"), lax.axis_index("col"), lax.axis_index("row")
    x, c = row // 2, row % 2
    rhs, rows, cols = x_ref.shape
    kcols = w_ref.shape[1]
    group = cols // SIDE

    def peer(k):
        kx, kc, kz = k // 4 % 2, k // 2 % 2, k % 2
        return x + kx * (1 - 2 * x), c + kc * (1 - 2 * c), z + kz * (1 - 2 * z)

    def device(k):
        px, pc, pz = peer(k)
        return (pz, j, px * 2 + pc)

    def in_side(k):
        _, pc, pz = peer(k)
        return pc * 2 + pz

    other_y = (z, 1 - j, row)

    def remote(src, dst, send, recv, to):
        return pltpu.make_async_remote_copy(src, dst, send, recv, device_id=to, device_id_type=MESH)

    def a_rows(k):
        return pl.ds(pl.multiple_of(in_side(k) * rows, rows), rows)

    def a_block(k, jj):
        return a_buf.at[a_rows(k), pl.ds(pl.multiple_of(jj * kcols, kcols), kcols)]

    def a_copy(n, receive=False):
        own = (w_ref, a_block(0, j))
        src, there, here, to = (
            own + (a_block(1, j), device(1)),
            own + (a_block(0, 1 - j), other_y),
            (a_block(1, j),) * 2 + (a_block(1, 1 - j), other_y),
            own + (a_block(2, j), device(2)),
            (a_block(1, j),) * 2 + (a_block(3, j), device(2)),
            (a_block(0, 1 - j),) * 2 + (a_block(2, 1 - j), device(2)),
            (a_block(1, 1 - j),) * 2 + (a_block(3, 1 - j), device(2)),
        )[n]
        return remote(src, here if receive else there, a_send.at[n], a_recv.at[n], to)

    def given(piece, k):
        r, at, width = piece
        return (r, slice(None), pl.ds(pl.multiple_of(in_side(k) * group + at, WIDE), width))

    def held(piece, k):
        r, at, width = piece
        px, pc, pz = peer(k)
        return x_buf.at[r, px, pc, pz, :, pl.ds(at, width)]

    def x_copy(piece, k, send, recv, receive=False):
        return remote(x_ref.at[given(piece, k)], held(piece, k if receive else 0), send, recv, device(k))

    def z_copy(n, i, receive=False):
        return x_copy(PIECES[n], (1, 3)[i], z_send.at[n, i], z_recv.at[n, i], receive)

    def d_copy(n, i, receive=False):
        return x_copy(DIRECT[n], (4, 6)[i], d_send.at[n, i], d_recv.at[n, i], receive)

    def f_copy(n, receive=False):
        r, at, width = PIECES[n]
        src = x_buf.at[r, x, :, 1 - z, :, pl.ds(at, width)]
        here = x_buf.at[r, 1 - x, :, 1 - z, :, pl.ds(at, width)]
        return remote(src, here if receive else src, f_send.at[n], f_recv.at[n], device(4))

    everything = (slice(None), 0, group)

    def p_copy(receive=False):
        return x_copy(everything, 2, p_send.at[0], p_recv.at[0], receive)

    def y_copy(n, kc, receive=False):
        k = kc * 2 + 1
        r, at, width = PIECES[n]
        src = y_buf.at[r, a_rows(k), pl.ds(at, width)]
        return remote(src, y_ref.at[given(PIECES[n], k if receive else 0)], y_send.at[n, kc], y_recv.at[n, kc], device(k))

    def q_copy(r, receive=False):
        piece = (r, 0, group)
        return remote(y_buf.at[r, a_rows(2), :], y_ref.at[given(piece, 2 if receive else 0)], q_send.at[r], q_recv.at[r], device(2))

    own_a = pltpu.make_async_copy(w_ref, a_block(0, j), own_sem.at[0])
    own_x = pltpu.make_async_copy(x_ref.at[given(everything, 0)], held(everything, 0), own_sem.at[1])

    def product(k, r, at):
        xs = x_buf[r, :, :, :, :, pl.ds(at, WIDE)].reshape(-1, WIDE)
        return jnp.dot(a_buf[a_rows(k), :], xs, preferred_element_type=jnp.float32).astype(y_buf.dtype)

    def forward(n):
        for i in range(2):
            z_copy(n, i, True).wait_recv()
        f_copy(n).start()

    def direct(n):
        for i in range(2):
            d_copy(n, i).start()

    def multiply(n):
        r, at, width = PIECES[n]
        for m, piece in enumerate(DIRECT):
            if piece[:2] == (r, at):
                for i in range(2):
                    d_copy(m, i, True).wait_recv()
        f_copy(n, True).wait_recv()
        parts = width // WIDE

        def tile(s, carry):
            t, at_s = s // parts, at + s % parts * WIDE
            kz = 1 - t // 2
            k = (t % 2 + t // 2) % 2 * 2 + kz
            at_s = pl.multiple_of(at_s, WIDE)
            y_buf[r, a_rows(k), pl.ds(at_s, WIDE)] = product(k, r, at_s)

            @pl.when(s % parts == 0)
            def _():
                for i in range(2):
                    @pl.when(t == i + 1)
                    def _():
                        y_copy(n, i).start()

            return carry

        lax.fori_loop(0, 3 * parts, tile, 0)

        def own(s, carry):
            at_s = pl.multiple_of(at + s * WIDE, WIDE)
            y_ref[r, :, pl.ds(pl.multiple_of(in_side(0) * group + at_s, WIDE), WIDE)] = product(0, r, at_s)
            return carry

        lax.fori_loop(0, parts, own, 0)
        if at + width == group:
            q_copy(r).start()

    barrier = pltpu.get_barrier_semaphore()
    for to in [device(k) for k in (1, 2, 3, 4, 6)] + [other_y]:
        pl.semaphore_signal(barrier, inc=1, device_id=to, device_id_type=MESH)
    pl.semaphore_wait(barrier, 6)

    a_copy(0).start()
    direct(0)
    a_copy(1).start()
    for n in range(len(PIECES)):
        for i in range(2):
            z_copy(n, i).start()
    direct(1)
    a_copy(3).start()
    own_a.start()
    p_copy().start()
    own_x.start()

    a_copy(0, True).wait_recv()
    a_copy(2).start()
    a_copy(4).start()
    a_copy(1, True).wait_recv()
    a_copy(5).start()
    forward(0)
    a_copy(2, True).wait_recv()
    a_copy(6).start()
    forward(1)
    own_a.wait()
    for n in (3, 4, 5, 6):
        a_copy(n, True).wait_recv()
    own_x.wait()
    p_copy(True).wait_recv()
    forward(2)
    multiply(0)
    forward(3)
    direct(2)
    multiply(1)
    forward(4)
    direct(3)
    multiply(2)
    forward(5)
    forward(6)
    for n in range(3, len(PIECES)):
        multiply(n)

    for n in range(7):
        a_copy(n).wait_send()
    p_copy().wait_send()
    for n in range(len(DIRECT)):
        for i in range(2):
            d_copy(n, i).wait_send()
    for n in range(len(PIECES)):
        f_copy(n).wait_send()
        for i in range(2):
            z_copy(n, i).wait_send()
    for r in range(rhs):
        q_copy(r).wait_send()
        q_copy(r, True).wait_recv()
    for n in range(len(PIECES)):
        for i in range(2):
            y_copy(n, i).wait_send()
            y_copy(n, i, True).wait_recv()


def solution(mesh):
    def local(w, x):
        rhs, rows, cols = x.shape
        n = w.shape[1] * 2
        sems = []
        for shape in ((7,), (len(PIECES), 2), (len(DIRECT), 2), (len(PIECES),), (1,), (len(PIECES), 2), (rhs,)):
            sems += [pltpu.SemaphoreType.DMA(shape)] * 2
        return pl.pallas_call(
            kernel,
            out_shape=pltpu.VMEM(x.shape, x.dtype),
            in_specs=[pl.BlockSpec(memory_space=pl.ANY)] * 2,
            out_specs=pl.BlockSpec(memory_space=pltpu.VMEM),
            scratch_shapes=[
                pltpu.VMEM((SIDE * rows, n), w.dtype),
                pltpu.VMEM((rhs, 2, 2, 2, rows, cols // SIDE), x.dtype),
                pltpu.VMEM((rhs, SIDE * rows, cols // SIDE), x.dtype),
                *sems,
                pltpu.SemaphoreType.DMA((2,)),
            ],
            compiler_params=pltpu.CompilerParams(collective_id=0, has_side_effects=True, vmem_limit_bytes=52 * 1024 * 1024),
        )(w, x)

    return jax.shard_map(local, mesh=mesh, in_specs=(P(("row", "depth"), "col"), P(None, ("row", "depth"), "col")),
                         out_specs=P(None, ("row", "depth"), "col"), check_vma=False)
```

```python
import jax
import jax.numpy as jnp
from jax import lax
from jax.experimental import pallas as pl
from jax.experimental.pallas import tpu as pltpu
from jax.sharding import PartitionSpec as P

MESH = pl.DeviceIdType.MESH
SIDE = 4
PIECES = ((0, 0, 1024), (1, 0, 1024), (2, 0, 512), (2, 512, 256), (2, 768, 256))
SPLIT = (0, 1)
WIDE = 256


def kernel(w_ref, x_ref, y_ref, a_buf, x_buf, y_buf, a_send, a_recv, z_send, z_recv, d_send, d_recv, f_send, f_recv,
           p_send, p_recv, y_send, y_recv, q_send, q_recv, own_sem):
    z, j, row = lax.axis_index("depth"), lax.axis_index("col"), lax.axis_index("row")
    x, c = row // 2, row % 2
    rhs, rows, cols = x_ref.shape
    kcols = w_ref.shape[1]
    group = cols // SIDE

    def peer(k):
        kx, kc, kz = k // 4 % 2, k // 2 % 2, k % 2
        return x + kx * (1 - 2 * x), c + kc * (1 - 2 * c), z + kz * (1 - 2 * z)

    def device(k):
        px, pc, pz = peer(k)
        return (pz, j, px * 2 + pc)

    def in_side(k):
        _, pc, pz = peer(k)
        return pc * 2 + pz

    other_y = (z, 1 - j, row)

    def remote(src, dst, send, recv, to):
        return pltpu.make_async_remote_copy(src, dst, send, recv, device_id=to, device_id_type=MESH)

    def a_rows(k):
        return pl.ds(pl.multiple_of(in_side(k) * rows, rows), rows)

    def a_block(k, jj):
        return a_buf.at[a_rows(k), pl.ds(pl.multiple_of(jj * kcols, kcols), kcols)]

    def a_copy(n, receive=False):
        own = (w_ref, a_block(0, j))
        src, there, here, to = (
            own + (a_block(1, j), device(1)),
            own + (a_block(0, 1 - j), other_y),
            (a_block(1, j),) * 2 + (a_block(1, 1 - j), other_y),
            own + (a_block(2, j), device(2)),
            (a_block(1, j),) * 2 + (a_block(3, j), device(2)),
            (a_block(0, 1 - j),) * 2 + (a_block(2, 1 - j), device(2)),
            (a_block(1, 1 - j),) * 2 + (a_block(3, 1 - j), device(2)),
        )[n]
        return remote(src, here if receive else there, a_send.at[n], a_recv.at[n], to)

    def given(piece, k):
        r, at, width = piece
        return (r, slice(None), pl.ds(pl.multiple_of(in_side(k) * group + at, WIDE), width))

    def held(piece, k):
        r, at, width = piece
        px, pc, pz = peer(k)
        return x_buf.at[r, px, pc, pz, :, pl.ds(at, width)]

    def x_copy(piece, k, send, recv, receive=False):
        return remote(x_ref.at[given(piece, k)], held(piece, k if receive else 0), send, recv, device(k))

    def z_copy(n, i, receive=False):
        return x_copy(PIECES[n], (1, 3)[i], z_send.at[n, i], z_recv.at[n, i], receive)

    def along_x(piece, side, send, recv, receive):
        r, at, width = piece
        src, here = (x_buf.at[r, px, :, side, :, pl.ds(at, width)] for px in (x, 1 - x))
        return remote(src, here if receive else src, send, recv, device(4))

    def d_copy(n, receive=False):
        if n == 0:
            return x_copy((0, 0, group), 4, d_send.at[n], d_recv.at[n], receive)
        if n == 1:
            src, here = (x_buf.at[0, px, 1 - c, z] for px in (x, 1 - x))
            return remote(src, here if receive else src, d_send.at[n], d_recv.at[n], device(4))
        return along_x((n - 1, 0, group), z, d_send.at[n], d_recv.at[n], receive)

    def f_copy(n, receive=False):
        side = 1 - z if PIECES[n][0] in SPLIT else slice(None)
        return along_x(PIECES[n], side, f_send.at[n], f_recv.at[n], receive)

    everything = (slice(None), 0, group)

    def p_copy(receive=False):
        return x_copy(everything, 2, p_send.at[0], p_recv.at[0], receive)

    def y_copy(n, kc, receive=False):
        k = kc * 2 + 1
        r, at, width = PIECES[n]
        src = y_buf.at[r, a_rows(k), pl.ds(at, width)]
        return remote(src, y_ref.at[given(PIECES[n], k if receive else 0)], y_send.at[n, kc], y_recv.at[n, kc], device(k))

    def q_copy(n, receive=False):
        r = (pl.ds(0, rhs - 1), pl.ds(rhs - 1, 1))[n]
        piece = (r, 0, group)
        return remote(y_buf.at[r, a_rows(2), :], y_ref.at[given(piece, 2 if receive else 0)], q_send.at[n], q_recv.at[n], device(2))

    own_a = pltpu.make_async_copy(w_ref, a_block(0, j), own_sem.at[0])
    own_x = pltpu.make_async_copy(x_ref.at[given(everything, 0)], held(everything, 0), own_sem.at[1])

    def product(k, r, at):
        xs = x_buf[r, :, :, :, :, pl.ds(at, WIDE)].reshape(-1, WIDE)
        return jnp.dot(a_buf[a_rows(k), :], xs, preferred_element_type=jnp.float32).astype(y_buf.dtype)

    def forward(n):
        for i in range(2):
            z_copy(n, i, True).wait_recv()
        f_copy(n).start()

    def multiply(n):
        r, at, width = PIECES[n]
        if r in SPLIT and at == 0:
            for m in (0, 1) if r == 0 else (r + 1,):
                d_copy(m, True).wait_recv()
        f_copy(n, True).wait_recv()
        parts = width // WIDE

        def tile(s, carry):
            t, at_s = s // parts, at + s % parts * WIDE
            kz = 1 - t // 2
            k = (t % 2 + t // 2) % 2 * 2 + kz
            at_s = pl.multiple_of(at_s, WIDE)
            y_buf[r, a_rows(k), pl.ds(at_s, WIDE)] = product(k, r, at_s)

            @pl.when(s % parts == 0)
            def _():
                for i in range(2):
                    @pl.when(t == i + 1)
                    def _():
                        y_copy(n, i).start()

            return carry

        lax.fori_loop(0, 3 * parts, tile, 0)

        def own(s, carry):
            at_s = pl.multiple_of(at + s * WIDE, WIDE)
            y_ref[r, :, pl.ds(pl.multiple_of(in_side(0) * group + at_s, WIDE), WIDE)] = product(0, r, at_s)
            return carry

        lax.fori_loop(0, parts, own, 0)
        if at + width == group and r >= rhs - 2:
            q_copy(r - rhs + 2).start()

    barrier = pltpu.get_barrier_semaphore()
    for to in [device(k) for k in (1, 2, 3, 4)] + [other_y]:
        pl.semaphore_signal(barrier, inc=1, device_id=to, device_id_type=MESH)
    pl.semaphore_wait(barrier, 5)

    a_copy(0).start()
    d_copy(0).start()
    p_copy().start()
    own_x.start()
    a_copy(1).start()
    for n in range(len(PIECES)):
        for i in range(2):
            z_copy(n, i).start()
    a_copy(3).start()
    own_a.start()

    own_x.wait()
    p_copy(True).wait_recv()
    for n in range(1, len(SPLIT) + 1):
        d_copy(n).start()
    a_copy(0, True).wait_recv()
    a_copy(2).start()
    a_copy(4).start()
    a_copy(1, True).wait_recv()
    a_copy(5).start()
    a_copy(2, True).wait_recv()
    a_copy(6).start()
    own_a.wait()
    for n in (3, 4, 5, 6):
        a_copy(n, True).wait_recv()
    forward(0)
    forward(1)
    multiply(0)
    forward(2)
    multiply(1)
    forward(3)
    forward(4)
    for n in range(2, len(PIECES)):
        multiply(n)

    for n in range(7):
        a_copy(n).wait_send()
    p_copy().wait_send()
    for n in range(len(SPLIT) + 1):
        d_copy(n).wait_send()
    for n in range(2):
        q_copy(n).wait_send()
        q_copy(n, True).wait_recv()
    for n in range(len(PIECES)):
        f_copy(n).wait_send()
        for i in range(2):
            z_copy(n, i).wait_send()
            y_copy(n, i).wait_send()
            y_copy(n, i, True).wait_recv()


def solution(mesh):
    def local(w, x):
        rhs, rows, cols = x.shape
        n = w.shape[1] * 2
        sems = []
        for shape in ((7,), (len(PIECES), 2), (len(SPLIT) + 1,), (len(PIECES),), (1,), (len(PIECES), 2), (2,)):
            sems += [pltpu.SemaphoreType.DMA(shape)] * 2
        return pl.pallas_call(
            kernel,
            out_shape=pltpu.VMEM(x.shape, x.dtype),
            in_specs=[pl.BlockSpec(memory_space=pl.ANY)] * 2,
            out_specs=pl.BlockSpec(memory_space=pltpu.VMEM),
            scratch_shapes=[
                pltpu.VMEM((SIDE * rows, n), w.dtype),
                pltpu.VMEM((rhs, 2, 2, 2, rows, cols // SIDE), x.dtype),
                pltpu.VMEM((rhs, SIDE * rows, cols // SIDE), x.dtype),
                *sems,
                pltpu.SemaphoreType.DMA((2,)),
            ],
            compiler_params=pltpu.CompilerParams(collective_id=0, has_side_effects=True, vmem_limit_bytes=52 * 1024 * 1024),
        )(w, x)

    return jax.shard_map(local, mesh=mesh, in_specs=(P(("row", "depth"), "col"), P(None, ("row", "depth"), "col")),
                         out_specs=P(None, ("row", "depth"), "col"), check_vma=False)
```

```python
import jax
import jax.numpy as jnp
from jax import lax
from jax.experimental import pallas as pl
from jax.experimental.pallas import tpu as pltpu
from jax.sharding import PartitionSpec as P

MESH = pl.DeviceIdType.MESH
SIDE = 4
PIECES = ((0, 0, 1024), (1, 0, 1024), (2, 0, 512), (2, 512, 256), (2, 768, 256))
SPLIT = 2
WIDE = 256


def kernel(w_ref, x_ref, y_ref, a_buf, x_buf, y_buf, a_send, a_recv, z_send, z_recv, d_send, d_recv, f_send, f_recv,
           p_send, p_recv, y_send, y_recv, q_send, q_recv, own_sem):
    z, j, row = lax.axis_index("depth"), lax.axis_index("col"), lax.axis_index("row")
    x, c = row // 2, row % 2
    rhs, rows, cols = x_ref.shape
    kcols = w_ref.shape[1]
    group = cols // SIDE

    def peer(k):
        kx, kc, kz = k // 4 % 2, k // 2 % 2, k % 2
        return x + kx * (1 - 2 * x), c + kc * (1 - 2 * c), z + kz * (1 - 2 * z)

    def device(k):
        px, pc, pz = peer(k)
        return (pz, j, px * 2 + pc)

    def in_side(k):
        _, pc, pz = peer(k)
        return pc * 2 + pz

    other_y = (z, 1 - j, row)

    def remote(src, dst, send, recv, to):
        return pltpu.make_async_remote_copy(src, dst, send, recv, device_id=to, device_id_type=MESH)

    def a_block(k, jj):
        _, pc, pz = peer(k)
        return a_buf.at[pc, pz, :, pl.ds(pl.multiple_of(jj * kcols, kcols), kcols)]

    def rows_of(k):
        return pl.ds(pl.multiple_of(in_side(k) * rows, rows), rows)

    def a_copy(n, receive=False):
        if n == 0:
            src, here, to = w_ref, a_block(1, j), device(1)
            there = a_block(0, j)
        elif n == 1:
            there, here = (a_buf.at[c, :, :, pl.ds(pl.multiple_of(jj * kcols, kcols), kcols)] for jj in (j, 1 - j))
            src, to = there, other_y
        else:
            there, here = a_buf.at[c], a_buf.at[1 - c]
            src, to = there, device(2)
        return remote(src, here if receive else there, a_send.at[n], a_recv.at[n], to)

    def given(piece, k):
        r, at, width = piece
        return (r, slice(None), pl.ds(pl.multiple_of(in_side(k) * group + at, WIDE), width))

    def held(piece, k):
        r, at, width = piece
        px, pc, pz = peer(k)
        return x_buf.at[r, px, pc, pz, :, pl.ds(at, width)]

    def x_copy(piece, k, send, recv, receive=False):
        return remote(x_ref.at[given(piece, k)], held(piece, k if receive else 0), send, recv, device(k))

    def z_copy(r, i, receive=False):
        return x_copy((r, 0, group), (1, 3)[i], z_send.at[r, i], z_recv.at[r, i], receive)

    def along_x(piece, side, send, recv, receive):
        r, at, width = piece
        src, here = (x_buf.at[r, px, :, side, :, pl.ds(at, width)] for px in (x, 1 - x))
        return remote(src, here if receive else src, send, recv, device(4))

    ahead = (pl.ds(0, SPLIT), 0, group)

    def d_copy(n, receive=False):
        if n == 0:
            return x_copy(ahead, 4, d_send.at[n], d_recv.at[n], receive)
        src, here = (x_buf.at[ahead[0], px, 1 - c, z] for px in (x, 1 - x))
        return remote(src, here if receive else src, d_send.at[n], d_recv.at[n], device(4))

    def f_copy(n, receive=False):
        side = 1 - z if PIECES[n][0] < SPLIT else slice(None)
        return along_x(PIECES[n], side, f_send.at[n], f_recv.at[n], receive)

    everything = (slice(None), 0, group)

    def p_copy(receive=False):
        return x_copy(everything, 2, p_send.at[0], p_recv.at[0], receive)

    def y_copy(n, kc, receive=False):
        k = kc * 2 + 1
        r, at, width = PIECES[n]
        src = y_buf.at[r, rows_of(k), pl.ds(at, width)]
        return remote(src, y_ref.at[given(PIECES[n], k if receive else 0)], y_send.at[n, kc], y_recv.at[n, kc], device(k))

    def q_copy(receive=False):
        there = y_ref.at[given(everything, 2 if receive else 0)]
        return remote(y_buf.at[:, rows_of(2), :], there, q_send.at[0], q_recv.at[0], device(2))

    own_a = pltpu.make_async_copy(w_ref, a_block(0, j), own_sem.at[0])
    own_x = pltpu.make_async_copy(x_ref.at[given(everything, 0)], held(everything, 0), own_sem.at[1])

    def product(k, r, at):
        xs = x_buf[r, :, :, :, :, pl.ds(at, WIDE)].reshape(-1, WIDE)
        return jnp.dot(a_buf[peer(k)[1], peer(k)[2]], xs, preferred_element_type=jnp.float32).astype(y_buf.dtype)

    def forward(n):
        r, at, _ = PIECES[n]
        if at == 0:
            for i in range(2):
                z_copy(r, i, True).wait_recv()
        f_copy(n).start()

    def multiply(n):
        r, at, width = PIECES[n]
        if n == 0:
            for m in range(2):
                d_copy(m, True).wait_recv()
        f_copy(n, True).wait_recv()
        parts = width // WIDE

        def tile(s, carry):
            t, at_s = s // parts, at + s % parts * WIDE
            kz = 1 - t // 2
            k = (t % 2 + t // 2) % 2 * 2 + kz
            at_s = pl.multiple_of(at_s, WIDE)
            y_buf[r, rows_of(k), pl.ds(at_s, WIDE)] = product(k, r, at_s)

            @pl.when(s % parts == 0)
            def _():
                for i in range(2):
                    @pl.when(t == i + 1)
                    def _():
                        y_copy(n, i).start()

            return carry

        lax.fori_loop(0, 3 * parts, tile, 0)

        def own(s, carry):
            at_s = pl.multiple_of(at + s * WIDE, WIDE)
            y_ref[r, :, pl.ds(pl.multiple_of(in_side(0) * group + at_s, WIDE), WIDE)] = product(0, r, at_s)
            return carry

        lax.fori_loop(0, parts, own, 0)

    barrier = pltpu.get_barrier_semaphore()
    for to in [device(k) for k in (1, 2, 3, 4)] + [other_y]:
        pl.semaphore_signal(barrier, inc=1, device_id=to, device_id_type=MESH)
    pl.semaphore_wait(barrier, 5)

    a_copy(0).start()
    d_copy(0).start()
    p_copy().start()
    own_x.start()
    for r in range(rhs):
        for i in range(2):
            z_copy(r, i).start()
    own_a.start()

    own_x.wait()
    p_copy(True).wait_recv()
    d_copy(1).start()
    own_a.wait()
    a_copy(0, True).wait_recv()
    a_copy(1).start()
    a_copy(1, True).wait_recv()
    a_copy(2).start()
    a_copy(2, True).wait_recv()
    forward(0)
    forward(1)
    multiply(0)
    forward(2)
    multiply(1)
    forward(3)
    forward(4)
    for n in range(2, len(PIECES)):
        multiply(n)

    q_copy().start()
    for n in range(3):
        a_copy(n).wait_send()
    p_copy().wait_send()
    for n in range(2):
        d_copy(n).wait_send()
    for r in range(rhs):
        for i in range(2):
            z_copy(r, i).wait_send()
    q_copy().wait_send()
    q_copy(True).wait_recv()
    for n in range(len(PIECES)):
        f_copy(n).wait_send()
        for i in range(2):
            y_copy(n, i).wait_send()
            y_copy(n, i, True).wait_recv()


def solution(mesh):
    def local(w, x):
        rhs, rows, cols = x.shape
        sems = []
        for shape in ((3,), (rhs, 2), (2,), (len(PIECES),), (1,), (len(PIECES), 2), (1,)):
            sems += [pltpu.SemaphoreType.DMA(shape)] * 2
        return pl.pallas_call(
            kernel,
            out_shape=pltpu.VMEM(x.shape, x.dtype),
            in_specs=[pl.BlockSpec(memory_space=pl.ANY)] * 2,
            out_specs=pl.BlockSpec(memory_space=pltpu.VMEM),
            scratch_shapes=[
                pltpu.VMEM((2, 2, rows, w.shape[1] * 2), w.dtype),
                pltpu.VMEM((rhs, 2, 2, 2, rows, cols // SIDE), x.dtype),
                pltpu.VMEM((rhs, SIDE * rows, cols // SIDE), x.dtype),
                *sems,
                pltpu.SemaphoreType.DMA((2,)),
            ],
            compiler_params=pltpu.CompilerParams(collective_id=0, has_side_effects=True, vmem_limit_bytes=52 * 1024 * 1024),
        )(w, x)

    return jax.shard_map(local, mesh=mesh, in_specs=(P(("row", "depth"), "col"), P(None, ("row", "depth"), "col")),
                         out_specs=P(None, ("row", "depth"), "col"), check_vma=False)
```

```python
import jax
import jax.numpy as jnp
from jax import lax
from jax.experimental import pallas as pl
from jax.experimental.pallas import tpu as pltpu
from jax.sharding import PartitionSpec as P

MESH = pl.DeviceIdType.MESH
SIDE = 4
PIECES = ((0, 0, 1024), (1, 0, 1024), (2, 0, 512), (2, 512, 256), (2, 768, 256))
SPLIT = 2
WIDE = 256


def kernel(w_ref, x_ref, y_ref, a_buf, x_buf, y_buf, a_send, a_recv, z_send, z_recv, d_send, d_recv, f_send, f_recv,
           p_send, p_recv, y_send, y_recv, q_send, q_recv, own_sem, ready):
    z, j, row = lax.axis_index("depth"), lax.axis_index("col"), lax.axis_index("row")
    x, c = row // 2, row % 2
    rhs, rows, cols = x_ref.shape
    kcols = w_ref.shape[1]
    group = cols // SIDE

    def peer(k):
        kx, kc, kz = k // 4 % 2, k // 2 % 2, k % 2
        return x + kx * (1 - 2 * x), c + kc * (1 - 2 * c), z + kz * (1 - 2 * z)

    def device(k):
        px, pc, pz = peer(k)
        return (pz, j, px * 2 + pc)

    def in_side(k):
        _, pc, pz = peer(k)
        return pc * 2 + pz

    other_y = (z, 1 - j, row)

    def remote(src, dst, send, recv, to):
        return pltpu.make_async_remote_copy(src, dst, send, recv, device_id=to, device_id_type=MESH)

    def a_block(k, jj):
        _, pc, pz = peer(k)
        return a_buf.at[pc, pz, :, pl.ds(pl.multiple_of(jj * kcols, kcols), kcols)]

    def rows_of(k):
        return pl.ds(pl.multiple_of(in_side(k) * rows, rows), rows)

    def a_copy(n, receive=False):
        if n == 0:
            src, here, to = w_ref, a_block(1, j), device(1)
            there = a_block(0, j)
        elif n == 1:
            there, here = (a_buf.at[c, :, :, pl.ds(pl.multiple_of(jj * kcols, kcols), kcols)] for jj in (j, 1 - j))
            src, to = there, other_y
        else:
            there, here = a_buf.at[c], a_buf.at[1 - c]
            src, to = there, device(2)
        return remote(src, here if receive else there, a_send.at[n], a_recv.at[n], to)

    def given(piece, k):
        r, at, width = piece
        return (r, slice(None), pl.ds(pl.multiple_of(in_side(k) * group + at, WIDE), width))

    def held(piece, k):
        r, at, width = piece
        px, pc, pz = peer(k)
        return x_buf.at[r, px, pc, pz, :, pl.ds(at, width)]

    def x_copy(piece, k, send, recv, receive=False):
        return remote(x_ref.at[given(piece, k)], held(piece, k if receive else 0), send, recv, device(k))

    def z_copy(r, i, receive=False):
        return x_copy((r, 0, group), (1, 3)[i], z_send.at[r, i], z_recv.at[r, i], receive)

    def along_x(piece, side, send, recv, receive):
        r, at, width = piece
        src, here = (x_buf.at[r, px, :, side, :, pl.ds(at, width)] for px in (x, 1 - x))
        return remote(src, here if receive else src, send, recv, device(4))

    ahead = (pl.ds(0, SPLIT), 0, group)

    def d_copy(n, receive=False):
        if n == 0:
            return x_copy(ahead, 4, d_send.at[n], d_recv.at[n], receive)
        src, here = (x_buf.at[ahead[0], px, 1 - c, z] for px in (x, 1 - x))
        return remote(src, here if receive else src, d_send.at[n], d_recv.at[n], device(4))

    def f_copy(n, receive=False):
        side = 1 - z if PIECES[n][0] < SPLIT else slice(None)
        return along_x(PIECES[n], side, f_send.at[n], f_recv.at[n], receive)

    everything = (slice(None), 0, group)

    def p_copy(receive=False):
        return x_copy(everything, 2, p_send.at[0], p_recv.at[0], receive)

    def y_copy(n, kc, receive=False):
        k = kc * 2 + 1
        r, at, width = PIECES[n]
        src = y_buf.at[r, rows_of(k), pl.ds(at, width)]
        return remote(src, y_ref.at[given(PIECES[n], k if receive else 0)], y_send.at[n, kc], y_recv.at[n, kc], device(k))

    def q_copy(receive=False):
        there = y_ref.at[given(everything, 2 if receive else 0)]
        return remote(y_buf.at[:, rows_of(2), :], there, q_send.at[0], q_recv.at[0], device(2))

    own_a = pltpu.make_async_copy(w_ref, a_block(0, j), own_sem.at[0])
    own_x = pltpu.make_async_copy(x_ref.at[given(everything, 0)], held(everything, 0), own_sem.at[1])

    def product(k, r, at):
        xs = x_buf[r, :, :, :, :, pl.ds(at, WIDE)].reshape(-1, WIDE)
        return jnp.dot(a_buf[peer(k)[1], peer(k)[2]], xs, preferred_element_type=jnp.float32).astype(y_buf.dtype)

    def forward(n):
        r, at, _ = PIECES[n]
        if at == 0:
            for i in range(2):
                z_copy(r, i, True).wait_recv()
        f_copy(n).start()

    def multiply(n):
        r, at, width = PIECES[n]
        if n == 0:
            for m in range(2):
                d_copy(m, True).wait_recv()
        f_copy(n, True).wait_recv()
        parts = width // WIDE

        def tile(s, carry):
            t, at_s = s // parts, at + s % parts * WIDE
            kz = 1 - t // 2
            k = (t % 2 + t // 2) % 2 * 2 + kz
            at_s = pl.multiple_of(at_s, WIDE)
            y_buf[r, rows_of(k), pl.ds(at_s, WIDE)] = product(k, r, at_s)

            @pl.when(s % parts == 0)
            def _():
                for i in range(2):
                    @pl.when(t == i + 1)
                    def _():
                        y_copy(n, i).start()

            return carry

        lax.fori_loop(0, 3 * parts, tile, 0)

        def own(s, carry):
            at_s = pl.multiple_of(at + s * WIDE, WIDE)
            y_ref[r, :, pl.ds(pl.multiple_of(in_side(0) * group + at_s, WIDE), WIDE)] = product(0, r, at_s)
            return carry

        lax.fori_loop(0, parts, own, 0)

    barrier = pltpu.get_barrier_semaphore()
    for k in (1, 3):
        pl.semaphore_signal(barrier, inc=1, device_id=device(k), device_id_type=MESH)

    @pl.when(z == 0)
    def _():
        for to in (device(2), device(4), other_y):
            pl.semaphore_signal(barrier, inc=1, device_id=to, device_id_type=MESH)
        pl.semaphore_wait(barrier, 5)
        for to in (device(4), other_y):
            pl.semaphore_signal(ready, inc=1, device_id=to, device_id_type=MESH)

    @pl.when(z == 1)
    def _():
        pl.semaphore_wait(barrier, 2)

    def beside_z():
        d_copy(0).start()
        p_copy().start()

    a_copy(0).start()
    pl.when(z == 0)(beside_z)
    for r in range(rhs):
        for i in range(2):
            z_copy(r, i).start()
    own_x.start()
    own_a.start()

    @pl.when(z == 0)
    def _():
        pl.semaphore_wait(ready, 2)
        pl.semaphore_signal(ready, inc=1, device_id=device(1), device_id_type=MESH)

    @pl.when(z == 1)
    def _():
        pl.semaphore_wait(ready, 1)
        beside_z()

    own_x.wait()
    p_copy(True).wait_recv()
    d_copy(1).start()
    own_a.wait()
    a_copy(0, True).wait_recv()
    a_copy(1).start()
    a_copy(1, True).wait_recv()
    a_copy(2).start()
    a_copy(2, True).wait_recv()
    forward(0)
    forward(1)
    multiply(0)
    forward(2)
    multiply(1)
    forward(3)
    forward(4)
    for n in range(2, len(PIECES)):
        multiply(n)

    q_copy().start()
    for n in range(3):
        a_copy(n).wait_send()
    p_copy().wait_send()
    for n in range(2):
        d_copy(n).wait_send()
    for r in range(rhs):
        for i in range(2):
            z_copy(r, i).wait_send()
    q_copy().wait_send()
    q_copy(True).wait_recv()
    for n in range(len(PIECES)):
        f_copy(n).wait_send()
        for i in range(2):
            y_copy(n, i).wait_send()
            y_copy(n, i, True).wait_recv()


def solution(mesh):
    def local(w, x):
        rhs, rows, cols = x.shape
        sems = []
        for shape in ((3,), (rhs, 2), (2,), (len(PIECES),), (1,), (len(PIECES), 2), (1,)):
            sems += [pltpu.SemaphoreType.DMA(shape)] * 2
        return pl.pallas_call(
            kernel,
            out_shape=pltpu.VMEM(x.shape, x.dtype),
            in_specs=[pl.BlockSpec(memory_space=pl.ANY)] * 2,
            out_specs=pl.BlockSpec(memory_space=pltpu.VMEM),
            scratch_shapes=[
                pltpu.VMEM((2, 2, rows, w.shape[1] * 2), w.dtype),
                pltpu.VMEM((rhs, 2, 2, 2, rows, cols // SIDE), x.dtype),
                pltpu.VMEM((rhs, SIDE * rows, cols // SIDE), x.dtype),
                *sems,
                pltpu.SemaphoreType.DMA((2,)),
                pltpu.SemaphoreType.REGULAR,
            ],
            compiler_params=pltpu.CompilerParams(collective_id=0, has_side_effects=True, vmem_limit_bytes=52 * 1024 * 1024),
        )(w, x)

    return jax.shard_map(local, mesh=mesh, in_specs=(P(("row", "depth"), "col"), P(None, ("row", "depth"), "col")),
                         out_specs=P(None, ("row", "depth"), "col"), check_vma=False)
```

```python
import jax
import jax.numpy as jnp
from jax import lax
from jax.experimental import pallas as pl
from jax.experimental.pallas import tpu as pltpu
from jax.sharding import PartitionSpec as P

MESH = pl.DeviceIdType.MESH
SIDE = 4
PIECES = ((0, 0, 1024), (1, 0, 1024), (2, 0, 512), (2, 512, 256), (2, 768, 256))
SPLIT = 2
WIDE = 256


def kernel(w_ref, x_ref, y_ref, a_buf, x_buf, y_buf, a_send, a_recv, in_send, in_recv, d_send, d_recv, f_send, f_recv,
           p_send, p_recv, y_send, y_recv, q_send, q_recv, own_sem, ready):
    z, j, row = lax.axis_index("depth"), lax.axis_index("col"), lax.axis_index("row")
    x, c = row // 2, row % 2
    rhs, rows, cols = x_ref.shape
    kcols = w_ref.shape[1]
    group = cols // SIDE

    def peer(k):
        kz, kc, kx = k // 4 % 2, k // 2 % 2, k % 2
        return x + kx * (1 - 2 * x), c + kc * (1 - 2 * c), z + kz * (1 - 2 * z)

    def device(k):
        px, pc, pz = peer(k)
        return (pz, j, px * 2 + pc)

    def in_side(k):
        px, pc, _ = peer(k)
        return pc * 2 + px

    other_y = (z, 1 - j, row)

    def remote(src, dst, send, recv, to):
        return pltpu.make_async_remote_copy(src, dst, send, recv, device_id=to, device_id_type=MESH)

    def a_block(k, jj):
        px, pc, _ = peer(k)
        return a_buf.at[pc, px, :, pl.ds(pl.multiple_of(jj * kcols, kcols), kcols)]

    def rows_of(k):
        return pl.ds(pl.multiple_of(in_side(k) * rows, rows), rows)

    def a_copy(n, receive=False):
        if n == 0:
            src, here, to = w_ref, a_block(1, j), device(1)
            there = a_block(0, j)
        elif n == 1:
            there, here = (a_buf.at[c, :, :, pl.ds(pl.multiple_of(jj * kcols, kcols), kcols)] for jj in (j, 1 - j))
            src, to = there, other_y
        else:
            there, here = a_buf.at[c], a_buf.at[1 - c]
            src, to = there, device(2)
        return remote(src, here if receive else there, a_send.at[n], a_recv.at[n], to)

    def given(piece, k):
        r, at, width = piece
        return (r, slice(None), pl.ds(pl.multiple_of(in_side(k) * group + at, WIDE), width))

    def held(piece, k):
        r, at, width = piece
        px, pc, pz = peer(k)
        return x_buf.at[r, px, pc, pz, :, pl.ds(at, width)]

    def x_copy(piece, k, send, recv, receive=False):
        return remote(x_ref.at[given(piece, k)], held(piece, k if receive else 0), send, recv, device(k))

    def in_copy(r, i, receive=False):
        return x_copy((r, 0, group), (1, 3)[i], in_send.at[r, i], in_recv.at[r, i], receive)

    def onward(piece, side, send, recv, receive):
        r, at, width = piece
        src, here = (x_buf.at[r, side, :, pz, :, pl.ds(at, width)] for pz in (z, 1 - z))
        return remote(src, here if receive else src, send, recv, device(4))

    ahead = (pl.ds(0, SPLIT), 0, group)

    def d_copy(n, receive=False):
        if n == 0:
            return x_copy(ahead, 4, d_send.at[n], d_recv.at[n], receive)
        src, here = (x_buf.at[ahead[0], x, 1 - c, pz] for pz in (z, 1 - z))
        return remote(src, here if receive else src, d_send.at[n], d_recv.at[n], device(4))

    def f_copy(n, receive=False):
        side = 1 - x if PIECES[n][0] < SPLIT else slice(None)
        return onward(PIECES[n], side, f_send.at[n], f_recv.at[n], receive)

    everything = (slice(None), 0, group)

    def p_copy(receive=False):
        return x_copy(everything, 2, p_send.at[0], p_recv.at[0], receive)

    def y_copy(n, kc, receive=False):
        k = kc * 2 + 1
        r, at, width = PIECES[n]
        src = y_buf.at[r, rows_of(k), pl.ds(at, width)]
        return remote(src, y_ref.at[given(PIECES[n], k if receive else 0)], y_send.at[n, kc], y_recv.at[n, kc], device(k))

    def q_copy(receive=False):
        there = y_ref.at[given(everything, 2 if receive else 0)]
        return remote(y_buf.at[:, rows_of(2), :], there, q_send.at[0], q_recv.at[0], device(2))

    own_a = pltpu.make_async_copy(w_ref, a_block(0, j), own_sem.at[0])
    own_x = pltpu.make_async_copy(x_ref.at[given(everything, 0)], held(everything, 0), own_sem.at[1])

    def product(k, r, at):
        xs = x_buf[r, :, :, :, :, pl.ds(at, WIDE)].reshape(-1, WIDE)
        return jnp.dot(a_buf[peer(k)[1], peer(k)[0]], xs, preferred_element_type=jnp.float32).astype(y_buf.dtype)

    def forward(n):
        r, at, _ = PIECES[n]
        if at == 0:
            for i in range(2):
                in_copy(r, i, True).wait_recv()
        f_copy(n).start()

    def multiply(n):
        r, at, width = PIECES[n]
        if n == 0:
            for m in range(2):
                d_copy(m, True).wait_recv()
        f_copy(n, True).wait_recv()
        parts = width // WIDE

        def tile(s, carry):
            t, at_s = s // parts, at + s % parts * WIDE
            kz = 1 - t // 2
            k = (t % 2 + t // 2) % 2 * 2 + kz
            at_s = pl.multiple_of(at_s, WIDE)
            y_buf[r, rows_of(k), pl.ds(at_s, WIDE)] = product(k, r, at_s)

            @pl.when(s % parts == 0)
            def _():
                for i in range(2):
                    @pl.when(t == i + 1)
                    def _():
                        y_copy(n, i).start()

            return carry

        lax.fori_loop(0, 3 * parts, tile, 0)

        def own(s, carry):
            at_s = pl.multiple_of(at + s * WIDE, WIDE)
            y_ref[r, :, pl.ds(pl.multiple_of(in_side(0) * group + at_s, WIDE), WIDE)] = product(0, r, at_s)
            return carry

        lax.fori_loop(0, parts, own, 0)

    barrier = pltpu.get_barrier_semaphore()
    for k in (1, 3):
        pl.semaphore_signal(barrier, inc=1, device_id=device(k), device_id_type=MESH)

    @pl.when(x == 0)
    def _():
        for to in (device(2), device(4), other_y):
            pl.semaphore_signal(barrier, inc=1, device_id=to, device_id_type=MESH)
        pl.semaphore_wait(barrier, 5)
        for to in (device(4), other_y):
            pl.semaphore_signal(ready, inc=1, device_id=to, device_id_type=MESH)

    @pl.when(x == 1)
    def _():
        pl.semaphore_wait(barrier, 2)

    def other_links():
        d_copy(0).start()
        p_copy().start()

    a_copy(0).start()
    pl.when(x == 0)(other_links)
    for r in range(rhs):
        for i in range(2):
            in_copy(r, i).start()
    own_x.start()
    own_a.start()

    @pl.when(x == 0)
    def _():
        pl.semaphore_wait(ready, 2)
        pl.semaphore_signal(ready, inc=1, device_id=device(1), device_id_type=MESH)

    @pl.when(x == 1)
    def _():
        pl.semaphore_wait(ready, 1)
        other_links()

    own_x.wait()
    p_copy(True).wait_recv()
    d_copy(1).start()
    own_a.wait()
    a_copy(0, True).wait_recv()
    a_copy(1).start()
    a_copy(1, True).wait_recv()
    a_copy(2).start()
    a_copy(2, True).wait_recv()
    forward(0)
    forward(1)
    multiply(0)
    forward(2)
    multiply(1)
    forward(3)
    forward(4)
    for n in range(2, len(PIECES)):
        multiply(n)

    q_copy().start()
    for n in range(3):
        a_copy(n).wait_send()
    p_copy().wait_send()
    for n in range(2):
        d_copy(n).wait_send()
    for r in range(rhs):
        for i in range(2):
            in_copy(r, i).wait_send()
    q_copy().wait_send()
    q_copy(True).wait_recv()
    for n in range(len(PIECES)):
        f_copy(n).wait_send()
        for i in range(2):
            y_copy(n, i).wait_send()
            y_copy(n, i, True).wait_recv()


def solution(mesh):
    def local(w, x):
        rhs, rows, cols = x.shape
        sems = []
        for shape in ((3,), (rhs, 2), (2,), (len(PIECES),), (1,), (len(PIECES), 2), (1,)):
            sems += [pltpu.SemaphoreType.DMA(shape)] * 2
        return pl.pallas_call(
            kernel,
            out_shape=pltpu.VMEM(x.shape, x.dtype),
            in_specs=[pl.BlockSpec(memory_space=pl.ANY)] * 2,
            out_specs=pl.BlockSpec(memory_space=pltpu.VMEM),
            scratch_shapes=[
                pltpu.VMEM((2, 2, rows, w.shape[1] * 2), w.dtype),
                pltpu.VMEM((rhs, 2, 2, 2, rows, cols // SIDE), x.dtype),
                pltpu.VMEM((rhs, SIDE * rows, cols // SIDE), x.dtype),
                *sems,
                pltpu.SemaphoreType.DMA((2,)),
                pltpu.SemaphoreType.REGULAR,
            ],
            compiler_params=pltpu.CompilerParams(collective_id=0, has_side_effects=True, vmem_limit_bytes=52 * 1024 * 1024),
        )(w, x)

    return jax.shard_map(local, mesh=mesh, in_specs=(P(("row", "depth"), "col"), P(None, ("row", "depth"), "col")),
                         out_specs=P(None, ("row", "depth"), "col"), check_vma=False)
```

```python
import functools

import jax
import jax.numpy as jnp
from jax import lax
from jax.experimental import pallas as pl
from jax.experimental.pallas import tpu as pltpu
from jax.sharding import PartitionSpec as P

MESH = pl.DeviceIdType.MESH
SIDE = 4
PIECES = ((0, 0, 1024), (1, 0, 1024), (2, 0, 512), (2, 512, 256), (2, 768, 256))
SPLIT = 2
WIDE = 256
MOVED = 16


def kernel(w_ref, x_ref, y_ref, a_buf, x_buf, y_buf, a_send, a_recv, in_send, in_recv, d_send, d_recv, f_send, f_recv,
           p_send, p_recv, y_send, y_recv, q_send, q_recv, own_sem, ready, e_buf, e_send, e_recv):
    z, j, row = lax.axis_index("depth"), lax.axis_index("col"), lax.axis_index("row")
    x, c = row // 2, row % 2
    rhs, rows, cols = x_ref.shape
    kcols = w_ref.shape[1]
    group = cols // SIDE

    def peer(k):
        kz, kc, kx = k // 4 % 2, k // 2 % 2, k % 2
        return x + kx * (1 - 2 * x), c + kc * (1 - 2 * c), z + kz * (1 - 2 * z)

    def device(k):
        px, pc, pz = peer(k)
        return (pz, j, px * 2 + pc)

    def in_side(k):
        px, pc, _ = peer(k)
        return pc * 2 + px

    other_y = (z, 1 - j, row)

    def remote(src, dst, send, recv, to):
        return pltpu.make_async_remote_copy(src, dst, send, recv, device_id=to, device_id_type=MESH)

    def a_block(k, jj):
        px, pc, _ = peer(k)
        return a_buf.at[pc, px, :, pl.ds(pl.multiple_of(jj * kcols, kcols), kcols)]

    def rows_of(k):
        return pl.ds(pl.multiple_of(in_side(k) * rows, rows), rows)

    def a_copy(n, receive=False):
        if n == 0:
            src, here, to = w_ref, a_block(1, j), device(1)
            there = a_block(0, j)
        elif n == 1:
            there, here = (a_buf.at[c, :, :, pl.ds(pl.multiple_of(jj * kcols, kcols), kcols)] for jj in (j, 1 - j))
            src, to = there, other_y
        else:
            there, here = a_buf.at[c], a_buf.at[1 - c]
            src, to = there, device(2)
        return remote(src, here if receive else there, a_send.at[n], a_recv.at[n], to)

    def a_over_x(op):
        few = (j == 0) & (c == 0)

        @pl.when(few)
        def _():
            rest = pl.ds(MOVED, rows - MOVED)
            src, there, here = w_ref.at[rest, :], a_block(0, j).at[rest, :], a_block(1, j).at[rest, :]
            op(lambda receive=False: remote(src, here if receive else there, a_send.at[0], a_recv.at[0], device(1)))

        @pl.when(jnp.logical_not(few))
        def _():
            op(lambda receive=False: a_copy(0, receive))

    def e_copy(n, receive=False):
        if n == 0:
            src, there, to = w_ref.at[pl.ds(0, MOVED), :], e_buf.at[0], other_y
        elif n == 1:
            src, there, to = e_buf.at[0], e_buf.at[1], device(1)
        else:
            src, there, to = e_buf.at[1], a_block(1, 0).at[pl.ds(0, MOVED), :], other_y
        return remote(src, there, e_send.at[n], e_recv.at[n], to)

    def when_moved(plane, body):
        pl.when((j == plane) & (c == 0))(body)

    def given(piece, k):
        r, at, width = piece
        return (r, slice(None), pl.ds(pl.multiple_of(in_side(k) * group + at, WIDE), width))

    def held(piece, k):
        r, at, width = piece
        px, pc, pz = peer(k)
        return x_buf.at[r, px, pc, pz, :, pl.ds(at, width)]

    def x_copy(piece, k, send, recv, receive=False):
        return remote(x_ref.at[given(piece, k)], held(piece, k if receive else 0), send, recv, device(k))

    def in_copy(r, i, receive=False):
        return x_copy((r, 0, group), (1, 3)[i], in_send.at[r, i], in_recv.at[r, i], receive)

    def onward(piece, side, send, recv, receive):
        r, at, width = piece
        src, here = (x_buf.at[r, side, :, pz, :, pl.ds(at, width)] for pz in (z, 1 - z))
        return remote(src, here if receive else src, send, recv, device(4))

    ahead = (pl.ds(0, SPLIT), 0, group)

    def d_copy(n, receive=False):
        if n == 0:
            return x_copy(ahead, 4, d_send.at[n], d_recv.at[n], receive)
        src, here = (x_buf.at[ahead[0], x, 1 - c, pz] for pz in (z, 1 - z))
        return remote(src, here if receive else src, d_send.at[n], d_recv.at[n], device(4))

    def f_copy(n, receive=False):
        side = 1 - x if PIECES[n][0] < SPLIT else slice(None)
        return onward(PIECES[n], side, f_send.at[n], f_recv.at[n], receive)

    everything = (slice(None), 0, group)

    def p_copy(receive=False):
        return x_copy(everything, 2, p_send.at[0], p_recv.at[0], receive)

    def y_copy(n, kc, receive=False):
        k = kc * 2 + 1
        r, at, width = PIECES[n]
        src = y_buf.at[r, rows_of(k), pl.ds(at, width)]
        return remote(src, y_ref.at[given(PIECES[n], k if receive else 0)], y_send.at[n, kc], y_recv.at[n, kc], device(k))

    def q_copy(receive=False):
        there = y_ref.at[given(everything, 2 if receive else 0)]
        return remote(y_buf.at[:, rows_of(2), :], there, q_send.at[0], q_recv.at[0], device(2))

    own_a = pltpu.make_async_copy(w_ref, a_block(0, j), own_sem.at[0])
    own_x = pltpu.make_async_copy(x_ref.at[given(everything, 0)], held(everything, 0), own_sem.at[1])

    def product(k, r, at):
        xs = x_buf[r, :, :, :, :, pl.ds(at, WIDE)].reshape(-1, WIDE)
        return jnp.dot(a_buf[peer(k)[1], peer(k)[0]], xs, preferred_element_type=jnp.float32).astype(y_buf.dtype)

    def forward(n):
        r, at, _ = PIECES[n]
        if at == 0:
            for i in range(2):
                in_copy(r, i, True).wait_recv()
        f_copy(n).start()

    def multiply(n):
        r, at, width = PIECES[n]
        if n == 0:
            for m in range(2):
                d_copy(m, True).wait_recv()
        f_copy(n, True).wait_recv()
        parts = width // WIDE

        def tile(s, carry):
            t, at_s = s // parts, at + s % parts * WIDE
            kz = 1 - t // 2
            k = (t % 2 + t // 2) % 2 * 2 + kz
            at_s = pl.multiple_of(at_s, WIDE)
            y_buf[r, rows_of(k), pl.ds(at_s, WIDE)] = product(k, r, at_s)

            @pl.when(s % parts == 0)
            def _():
                for i in range(2):
                    @pl.when(t == i + 1)
                    def _():
                        y_copy(n, i).start()

            return carry

        lax.fori_loop(0, 3 * parts, tile, 0)

        def own(s, carry):
            at_s = pl.multiple_of(at + s * WIDE, WIDE)
            y_ref[r, :, pl.ds(pl.multiple_of(in_side(0) * group + at_s, WIDE), WIDE)] = product(0, r, at_s)
            return carry

        lax.fori_loop(0, parts, own, 0)

    barrier = pltpu.get_barrier_semaphore()
    for k in (1, 3):
        pl.semaphore_signal(barrier, inc=1, device_id=device(k), device_id_type=MESH)

    @pl.when(x == 0)
    def _():
        for to in (device(2), device(4), other_y):
            pl.semaphore_signal(barrier, inc=1, device_id=to, device_id_type=MESH)
        pl.semaphore_wait(barrier, 5)
        for to in (device(4), other_y):
            pl.semaphore_signal(ready, inc=1, device_id=to, device_id_type=MESH)

    @pl.when(x == 1)
    def _():
        pl.semaphore_wait(barrier, 2)

    def other_links():
        d_copy(0).start()
        p_copy().start()

    a_over_x(lambda copy: copy().start())
    pl.when(x == 0)(other_links)
    own_x.start()
    own_a.start()

    @pl.when(x == 0)
    def _():
        pl.semaphore_wait(ready, 2)
        pl.semaphore_signal(ready, inc=1, device_id=device(1), device_id_type=MESH)

    @pl.when(x == 1)
    def _():
        pl.semaphore_wait(ready, 1)
        other_links()

    when_moved(0, lambda: e_copy(0).start())

    @functools.partial(when_moved, 1)
    def _():
        e_copy(0, True).wait_recv()
        e_copy(1).start()

    for r in range(rhs):
        for i in range(2):
            in_copy(r, i).start()
    own_x.wait()
    p_copy(True).wait_recv()
    d_copy(1).start()
    own_a.wait()
    a_over_x(lambda copy: copy(True).wait_recv())

    @functools.partial(when_moved, 1)
    def _():
        e_copy(1, True).wait_recv()
        e_copy(2).start()

    when_moved(0, lambda: e_copy(2, True).wait_recv())
    a_copy(1).start()
    a_copy(1, True).wait_recv()
    a_copy(2).start()
    a_copy(2, True).wait_recv()
    forward(0)
    forward(1)
    multiply(0)
    forward(2)
    multiply(1)
    forward(3)
    forward(4)
    for n in range(2, len(PIECES)):
        multiply(n)

    q_copy().start()
    a_over_x(lambda copy: copy().wait_send())
    when_moved(0, lambda: e_copy(0).wait_send())

    @functools.partial(when_moved, 1)
    def _():
        e_copy(1).wait_send()
        e_copy(2).wait_send()

    for n in range(1, 3):
        a_copy(n).wait_send()
    p_copy().wait_send()
    for n in range(2):
        d_copy(n).wait_send()
    for r in range(rhs):
        for i in range(2):
            in_copy(r, i).wait_send()
    q_copy().wait_send()
    q_copy(True).wait_recv()
    for n in range(len(PIECES)):
        f_copy(n).wait_send()
        for i in range(2):
            y_copy(n, i).wait_send()
            y_copy(n, i, True).wait_recv()


def solution(mesh):
    def local(w, x):
        rhs, rows, cols = x.shape
        sems = []
        for shape in ((3,), (rhs, 2), (2,), (len(PIECES),), (1,), (len(PIECES), 2), (1,)):
            sems += [pltpu.SemaphoreType.DMA(shape)] * 2
        return pl.pallas_call(
            kernel,
            out_shape=pltpu.VMEM(x.shape, x.dtype),
            in_specs=[pl.BlockSpec(memory_space=pl.ANY)] * 2,
            out_specs=pl.BlockSpec(memory_space=pltpu.VMEM),
            scratch_shapes=[
                pltpu.VMEM((2, 2, rows, w.shape[1] * 2), w.dtype),
                pltpu.VMEM((rhs, 2, 2, 2, rows, cols // SIDE), x.dtype),
                pltpu.VMEM((rhs, SIDE * rows, cols // SIDE), x.dtype),
                *sems,
                pltpu.SemaphoreType.DMA((2,)),
                pltpu.SemaphoreType.REGULAR,
                pltpu.VMEM((2, MOVED, w.shape[1]), w.dtype),
                pltpu.SemaphoreType.DMA((3,)),
                pltpu.SemaphoreType.DMA((3,)),
            ],
            compiler_params=pltpu.CompilerParams(collective_id=0, has_side_effects=True, vmem_limit_bytes=52 * 1024 * 1024),
        )(w, x)

    return jax.shard_map(local, mesh=mesh, in_specs=(P(("row", "depth"), "col"), P(None, ("row", "depth"), "col")),
                         out_specs=P(None, ("row", "depth"), "col"), check_vma=False)
```

```python
import functools

import jax
import jax.numpy as jnp
from jax import lax
from jax.experimental import pallas as pl
from jax.experimental.pallas import tpu as pltpu
from jax.sharding import PartitionSpec as P

MESH = pl.DeviceIdType.MESH
SIDE = 4
PIECES = ((0, 0, 1024), (1, 0, 1024), (2, 0, 512), (2, 512, 256), (2, 768, 256))
SPLIT = 2
WIDE = 256
MOVED = 16


def kernel(w_ref, x_ref, y_ref, a_buf, x_buf, y_buf, a_send, a_recv, in_send, in_recv, d_send, d_recv, f_send, f_recv,
           p_send, p_recv, y_send, y_recv, q_send, q_recv, own_sem, ready, e_buf, e_send, e_recv):
    z, j, row = lax.axis_index("depth"), lax.axis_index("col"), lax.axis_index("row")
    x, c = row // 2, row % 2
    rhs, rows, cols = x_ref.shape
    kcols = w_ref.shape[1]
    group = cols // SIDE

    def peer(k):
        kz, kc, kx = k // 4 % 2, k // 2 % 2, k % 2
        return x + kx * (1 - 2 * x), c + kc * (1 - 2 * c), z + kz * (1 - 2 * z)

    def device(k):
        px, pc, pz = peer(k)
        return (pz, j, px * 2 + pc)

    def in_side(k):
        px, pc, _ = peer(k)
        return pc * 2 + px

    other_y = (z, 1 - j, row)

    def remote(src, dst, send, recv, to):
        return pltpu.make_async_remote_copy(src, dst, send, recv, device_id=to, device_id_type=MESH)

    def a_block(k, jj):
        px, pc, _ = peer(k)
        return a_buf.at[pc, px, :, pl.ds(pl.multiple_of(jj * kcols, kcols), kcols)]

    def rows_of(k):
        return pl.ds(pl.multiple_of(in_side(k) * rows, rows), rows)

    def a_copy(n, receive=False):
        if n == 0:
            src, here, to = w_ref, a_block(1, j), device(1)
            there = a_block(0, j)
        elif n == 1:
            there, here = (a_buf.at[c, :, :, pl.ds(pl.multiple_of(jj * kcols, kcols), kcols)] for jj in (j, 1 - j))
            src, to = there, other_y
        else:
            there, here = a_buf.at[c], a_buf.at[1 - c]
            src, to = there, device(2)
        return remote(src, here if receive else there, a_send.at[n], a_recv.at[n], to)

    def a_over_x(op):
        few = (j == 0) & (c == 0)

        @pl.when(few)
        def _():
            rest = pl.ds(MOVED, rows - MOVED)
            src, there, here = w_ref.at[rest, :], a_block(0, j).at[rest, :], a_block(1, j).at[rest, :]
            op(lambda receive=False: remote(src, here if receive else there, a_send.at[0], a_recv.at[0], device(1)))

        @pl.when(jnp.logical_not(few))
        def _():
            op(lambda receive=False: a_copy(0, receive))

    def e_copy(n, receive=False):
        if n == 0:
            src, there, to = w_ref.at[pl.ds(0, MOVED), :], e_buf.at[0], other_y
        elif n == 1:
            src, there, to = e_buf.at[0], e_buf.at[1], device(1)
        else:
            src, there, to = e_buf.at[1], a_block(1, 0).at[pl.ds(0, MOVED), :], other_y
        return remote(src, there, e_send.at[n], e_recv.at[n], to)

    def when_moved(plane, body):
        pl.when((j == plane) & (c == 0))(body)

    def given(piece, k):
        r, at, width = piece
        return (r, slice(None), pl.ds(pl.multiple_of(in_side(k) * group + at, WIDE), width))

    def held(piece, k):
        r, at, width = piece
        px, pc, pz = peer(k)
        return x_buf.at[r, px, pc, pz, :, pl.ds(at, width)]

    def x_copy(piece, k, send, recv, receive=False):
        return remote(x_ref.at[given(piece, k)], held(piece, k if receive else 0), send, recv, device(k))

    def in_copy(r, i, receive=False):
        return x_copy((r, 0, group), (1, 3)[i], in_send.at[r, i], in_recv.at[r, i], receive)

    def onward(piece, side, send, recv, receive):
        r, at, width = piece
        src, here = (x_buf.at[r, side, :, pz, :, pl.ds(at, width)] for pz in (z, 1 - z))
        return remote(src, here if receive else src, send, recv, device(4))

    ahead = (pl.ds(0, SPLIT), 0, group)

    def d_copy(n, receive=False):
        if n == 0:
            return x_copy(ahead, 4, d_send.at[n], d_recv.at[n], receive)
        src, here = (x_buf.at[ahead[0], x, 1 - c, pz] for pz in (z, 1 - z))
        return remote(src, here if receive else src, d_send.at[n], d_recv.at[n], device(4))

    def f_copy(n, receive=False):
        side = 1 - x if PIECES[n][0] < SPLIT else slice(None)
        return onward(PIECES[n], side, f_send.at[n], f_recv.at[n], receive)

    everything = (slice(None), 0, group)

    def p_copy(receive=False):
        return x_copy(everything, 2, p_send.at[0], p_recv.at[0], receive)

    def y_copy(n, kc, receive=False):
        k = kc * 2 + 1
        r, at, width = PIECES[n]
        src = y_buf.at[r, rows_of(k), pl.ds(at, width)]
        return remote(src, y_ref.at[given(PIECES[n], k if receive else 0)], y_send.at[n, kc], y_recv.at[n, kc], device(k))

    def q_copy(receive=False):
        there = y_ref.at[given(everything, 2 if receive else 0)]
        return remote(y_buf.at[:, rows_of(2), :], there, q_send.at[0], q_recv.at[0], device(2))

    own_a = pltpu.make_async_copy(w_ref, a_block(0, j), own_sem.at[0])
    own_x = pltpu.make_async_copy(x_ref.at[given(everything, 0)], held(everything, 0), own_sem.at[1])

    def product(k, r, at):
        xs = x_buf[r, :, :, :, :, pl.ds(at, WIDE)].reshape(-1, WIDE)
        return jnp.dot(a_buf[peer(k)[1], peer(k)[0]], xs, preferred_element_type=jnp.float32).astype(y_buf.dtype)

    def forward(n):
        r, at, _ = PIECES[n]
        if at == 0:
            for i in range(2):
                in_copy(r, i, True).wait_recv()
        f_copy(n).start()

    def multiply(n):
        r, at, width = PIECES[n]
        if n == 0:
            for m in range(2):
                d_copy(m, True).wait_recv()
        f_copy(n, True).wait_recv()
        parts = width // WIDE

        def tile(s, carry):
            t, at_s = s // parts, at + s % parts * WIDE
            kz = 1 - t // 2
            k = (t % 2 + t // 2) % 2 * 2 + kz
            at_s = pl.multiple_of(at_s, WIDE)
            y_buf[r, rows_of(k), pl.ds(at_s, WIDE)] = product(k, r, at_s)

            @pl.when(s % parts == 0)
            def _():
                for i in range(2):
                    @pl.when(t == i + 1)
                    def _():
                        y_copy(n, i).start()

            return carry

        lax.fori_loop(0, 3 * parts, tile, 0)

        def own(s, carry):
            at_s = pl.multiple_of(at + s * WIDE, WIDE)
            y_ref[r, :, pl.ds(pl.multiple_of(in_side(0) * group + at_s, WIDE), WIDE)] = product(0, r, at_s)
            return carry

        lax.fori_loop(0, parts, own, 0)

    barrier = pltpu.get_barrier_semaphore()
    pl.semaphore_signal(barrier, inc=1, device_id=device(1), device_id_type=MESH)
    beside = (device(4), other_y, device(2))

    @pl.when(x == 0)
    def _():
        for to in beside:
            pl.semaphore_signal(barrier, inc=1, device_id=to, device_id_type=MESH)
        pl.semaphore_wait(barrier, 4)
        for to in beside:
            pl.semaphore_signal(ready, inc=1, device_id=to, device_id_type=MESH)

    @pl.when(x == 1)
    def _():
        pl.semaphore_wait(barrier, 1)

    def other_links():
        d_copy(0).start()
        p_copy().start()

    a_over_x(lambda copy: copy().start())
    pl.when(x == 0)(other_links)
    own_x.start()
    own_a.start()

    @pl.when(x == 0)
    def _():
        pl.semaphore_wait(ready, 3)
        pl.semaphore_signal(ready, inc=1, device_id=device(1), device_id_type=MESH)

    @pl.when(x == 1)
    def _():
        pl.semaphore_wait(ready, 1)
        other_links()

    when_moved(0, lambda: e_copy(0).start())

    @functools.partial(when_moved, 1)
    def _():
        e_copy(0, True).wait_recv()
        e_copy(1).start()

    for r in range(rhs):
        for i in range(2):
            in_copy(r, i).start()
    own_x.wait()
    p_copy(True).wait_recv()
    d_copy(1).start()
    own_a.wait()
    a_over_x(lambda copy: copy(True).wait_recv())

    @functools.partial(when_moved, 1)
    def _():
        e_copy(1, True).wait_recv()
        e_copy(2).start()

    when_moved(0, lambda: e_copy(2, True).wait_recv())
    a_copy(1).start()
    a_copy(1, True).wait_recv()
    a_copy(2).start()
    a_copy(2, True).wait_recv()
    forward(0)
    forward(1)
    multiply(0)
    forward(2)
    multiply(1)
    forward(3)
    forward(4)
    for n in range(2, len(PIECES)):
        multiply(n)

    q_copy().start()
    a_over_x(lambda copy: copy().wait_send())
    when_moved(0, lambda: e_copy(0).wait_send())

    @functools.partial(when_moved, 1)
    def _():
        e_copy(1).wait_send()
        e_copy(2).wait_send()

    for n in range(1, 3):
        a_copy(n).wait_send()
    p_copy().wait_send()
    for n in range(2):
        d_copy(n).wait_send()
    for r in range(rhs):
        for i in range(2):
            in_copy(r, i).wait_send()
    q_copy().wait_send()
    q_copy(True).wait_recv()
    for n in range(len(PIECES)):
        f_copy(n).wait_send()
        for i in range(2):
            y_copy(n, i).wait_send()
            y_copy(n, i, True).wait_recv()


def solution(mesh):
    def local(w, x):
        rhs, rows, cols = x.shape
        sems = []
        for shape in ((3,), (rhs, 2), (2,), (len(PIECES),), (1,), (len(PIECES), 2), (1,)):
            sems += [pltpu.SemaphoreType.DMA(shape)] * 2
        return pl.pallas_call(
            kernel,
            out_shape=pltpu.VMEM(x.shape, x.dtype),
            in_specs=[pl.BlockSpec(memory_space=pl.ANY)] * 2,
            out_specs=pl.BlockSpec(memory_space=pltpu.VMEM),
            scratch_shapes=[
                pltpu.VMEM((2, 2, rows, w.shape[1] * 2), w.dtype),
                pltpu.VMEM((rhs, 2, 2, 2, rows, cols // SIDE), x.dtype),
                pltpu.VMEM((rhs, SIDE * rows, cols // SIDE), x.dtype),
                *sems,
                pltpu.SemaphoreType.DMA((2,)),
                pltpu.SemaphoreType.REGULAR,
                pltpu.VMEM((2, MOVED, w.shape[1]), w.dtype),
                pltpu.SemaphoreType.DMA((3,)),
                pltpu.SemaphoreType.DMA((3,)),
            ],
            compiler_params=pltpu.CompilerParams(collective_id=0, has_side_effects=True, vmem_limit_bytes=52 * 1024 * 1024),
        )(w, x)

    return jax.shard_map(local, mesh=mesh, in_specs=(P(("row", "depth"), "col"), P(None, ("row", "depth"), "col")),
                         out_specs=P(None, ("row", "depth"), "col"), check_vma=False)
```

```python
import functools

import jax
import jax.numpy as jnp
from jax import lax
from jax.experimental import pallas as pl
from jax.experimental.pallas import tpu as pltpu
from jax.sharding import PartitionSpec as P

MESH = pl.DeviceIdType.MESH
SIDE = 4
PIECES = ((0, 0, 1024), (1, 0, 1024), (2, 0, 512), (2, 512, 256), (2, 768, 256))
SPLIT = 2
WIDE = 256
MOVED = 16


def kernel(w_ref, x_ref, y_ref, a_buf, x_buf, y_buf, a_send, a_recv, in_send, in_recv, d_send, d_recv, f_send, f_recv,
           p_send, p_recv, y_send, y_recv, q_send, q_recv, own_sem, ready, e_buf, e_send, e_recv):
    z, j, row = lax.axis_index("depth"), lax.axis_index("col"), lax.axis_index("row")
    x, c = row // 2, row % 2
    rhs, rows, cols = x_ref.shape
    kcols = w_ref.shape[1]
    group = cols // SIDE

    def peer(k):
        kz, kc, kx = k // 4 % 2, k // 2 % 2, k % 2
        return x + kx * (1 - 2 * x), c + kc * (1 - 2 * c), z + kz * (1 - 2 * z)

    def device(k):
        px, pc, pz = peer(k)
        return (pz, j, px * 2 + pc)

    def in_side(k):
        px, pc, _ = peer(k)
        return pc * 2 + px

    other_y = (z, 1 - j, row)

    def remote(src, dst, send, recv, to):
        return pltpu.make_async_remote_copy(src, dst, send, recv, device_id=to, device_id_type=MESH)

    def a_block(k, jj):
        px, pc, _ = peer(k)
        return a_buf.at[pc, px, :, pl.ds(pl.multiple_of(jj * kcols, kcols), kcols)]

    def rows_of(k):
        return pl.ds(pl.multiple_of(in_side(k) * rows, rows), rows)

    def a_copy(n, receive=False):
        if n == 0:
            src, here, to = w_ref, a_block(1, j), device(1)
            there = a_block(0, j)
        elif n == 1:
            there, here = (a_buf.at[c, :, :, pl.ds(pl.multiple_of(jj * kcols, kcols), kcols)] for jj in (j, 1 - j))
            src, to = there, other_y
        else:
            there, here = a_buf.at[c], a_buf.at[1 - c]
            src, to = there, device(2)
        return remote(src, here if receive else there, a_send.at[n], a_recv.at[n], to)

    def a_over_x(op):
        few = (j == 0) & (c == 0)

        @pl.when(few)
        def _():
            rest = pl.ds(MOVED, rows - MOVED)
            src, there, here = w_ref.at[rest, :], a_block(0, j).at[rest, :], a_block(1, j).at[rest, :]
            op(lambda receive=False: remote(src, here if receive else there, a_send.at[0], a_recv.at[0], device(1)))

        @pl.when(jnp.logical_not(few))
        def _():
            op(lambda receive=False: a_copy(0, receive))

    def e_copy(n, receive=False):
        if n == 0:
            src, there, to = w_ref.at[pl.ds(0, MOVED), :], e_buf.at[0], other_y
        elif n == 1:
            src, there, to = e_buf.at[0], e_buf.at[1], device(1)
        else:
            src, there, to = e_buf.at[1], a_block(1, 0).at[pl.ds(0, MOVED), :], other_y
        return remote(src, there, e_send.at[n], e_recv.at[n], to)

    def when_moved(plane, body):
        pl.when((j == plane) & (c == 0))(body)

    def given(piece, k):
        r, at, width = piece
        return (r, slice(None), pl.ds(pl.multiple_of(in_side(k) * group + at, WIDE), width))

    def held(piece, k):
        r, at, width = piece
        px, pc, pz = peer(k)
        return x_buf.at[r, px, pc, pz, :, pl.ds(at, width)]

    def x_copy(piece, k, send, recv, receive=False):
        return remote(x_ref.at[given(piece, k)], held(piece, k if receive else 0), send, recv, device(k))

    def in_copy(r, i, receive=False):
        return x_copy((r, 0, group), (1, 3)[i], in_send.at[r, i], in_recv.at[r, i], receive)

    def onward(piece, side, send, recv, receive):
        r, at, width = piece
        src, here = (x_buf.at[r, side, :, pz, :, pl.ds(at, width)] for pz in (z, 1 - z))
        return remote(src, here if receive else src, send, recv, device(4))

    ahead = (pl.ds(0, SPLIT), 0, group)

    def d_copy(n, receive=False):
        if n == 0:
            return x_copy(ahead, 4, d_send.at[n], d_recv.at[n], receive)
        src, here = (x_buf.at[ahead[0], x, 1 - c, pz] for pz in (z, 1 - z))
        return remote(src, here if receive else src, d_send.at[n], d_recv.at[n], device(4))

    def f_copy(n, receive=False):
        side = 1 - x if PIECES[n][0] < SPLIT else slice(None)
        return onward(PIECES[n], side, f_send.at[n], f_recv.at[n], receive)

    everything = (slice(None), 0, group)

    def p_copy(receive=False):
        return x_copy(everything, 2, p_send.at[0], p_recv.at[0], receive)

    def y_copy(n, kc, receive=False):
        k = kc * 2 + 1
        r, at, width = PIECES[n]
        src = y_buf.at[r, rows_of(k), pl.ds(at, width)]
        return remote(src, y_ref.at[given(PIECES[n], k if receive else 0)], y_send.at[n, kc], y_recv.at[n, kc], device(k))

    def q_copy(receive=False):
        there = y_ref.at[given(everything, 2 if receive else 0)]
        return remote(y_buf.at[:, rows_of(2), :], there, q_send.at[0], q_recv.at[0], device(2))

    own_a = pltpu.make_async_copy(w_ref, a_block(0, j), own_sem.at[0])
    own_x = pltpu.make_async_copy(x_ref.at[given(everything, 0)], held(everything, 0), own_sem.at[1])

    def product(k, r, at):
        xs = x_buf[r, :, :, :, :, pl.ds(at, WIDE)].reshape(-1, WIDE)
        return jnp.dot(a_buf[peer(k)[1], peer(k)[0]], xs, preferred_element_type=jnp.float32).astype(y_buf.dtype)

    def forward(n):
        r, at, _ = PIECES[n]
        if at == 0:
            for i in range(2):
                in_copy(r, i, True).wait_recv()
        f_copy(n).start()

    def multiply(n):
        r, at, width = PIECES[n]
        if n == 0:
            for m in range(2):
                d_copy(m, True).wait_recv()
        f_copy(n, True).wait_recv()
        parts = width // WIDE

        def tile(s, carry):
            t, at_s = s // parts, at + s % parts * WIDE
            kz = 1 - t // 2
            k = (t % 2 + t // 2) % 2 * 2 + kz
            at_s = pl.multiple_of(at_s, WIDE)
            y_buf[r, rows_of(k), pl.ds(at_s, WIDE)] = product(k, r, at_s)

            @pl.when(s % parts == 0)
            def _():
                for i in range(2):
                    @pl.when(t == i + 1)
                    def _():
                        y_copy(n, i).start()

            return carry

        lax.fori_loop(0, 3 * parts, tile, 0)

        def own(s, carry):
            at_s = pl.multiple_of(at + s * WIDE, WIDE)
            y_ref[r, :, pl.ds(pl.multiple_of(in_side(0) * group + at_s, WIDE), WIDE)] = product(0, r, at_s)
            return carry

        lax.fori_loop(0, parts, own, 0)

    barrier = pltpu.get_barrier_semaphore()
    pl.semaphore_signal(barrier, inc=1, device_id=device(1), device_id_type=MESH)
    beside = (device(4), other_y, device(2))
    own_x.start()
    own_a.start()

    @pl.when(x == 0)
    def _():
        for to in beside:
            pl.semaphore_signal(barrier, inc=1, device_id=to, device_id_type=MESH)
        pl.semaphore_wait(barrier, 4)
        for to in beside:
            pl.semaphore_signal(ready, inc=1, device_id=to, device_id_type=MESH)

    @pl.when(x == 1)
    def _():
        pl.semaphore_wait(barrier, 1)

    def other_links():
        d_copy(0).start()
        p_copy().start()

    a_over_x(lambda copy: copy().start())
    pl.when(x == 0)(other_links)

    @pl.when(x == 0)
    def _():
        pl.semaphore_wait(ready, 3)
        pl.semaphore_signal(ready, inc=1, device_id=device(1), device_id_type=MESH)

    @pl.when(x == 1)
    def _():
        pl.semaphore_wait(ready, 1)
        other_links()

    when_moved(0, lambda: e_copy(0).start())

    @functools.partial(when_moved, 1)
    def _():
        e_copy(0, True).wait_recv()
        e_copy(1).start()

    for r in range(rhs):
        for i in range(2):
            in_copy(r, i).start()
    own_x.wait()
    p_copy(True).wait_recv()
    d_copy(1).start()
    own_a.wait()
    a_over_x(lambda copy: copy(True).wait_recv())

    @functools.partial(when_moved, 1)
    def _():
        e_copy(1, True).wait_recv()
        e_copy(2).start()

    when_moved(0, lambda: e_copy(2, True).wait_recv())
    a_copy(1).start()
    a_copy(1, True).wait_recv()
    a_copy(2).start()
    a_copy(2, True).wait_recv()
    forward(0)
    forward(1)
    multiply(0)
    forward(2)
    multiply(1)
    forward(3)
    forward(4)
    for n in range(2, len(PIECES)):
        multiply(n)

    q_copy().start()
    a_over_x(lambda copy: copy().wait_send())
    when_moved(0, lambda: e_copy(0).wait_send())

    @functools.partial(when_moved, 1)
    def _():
        e_copy(1).wait_send()
        e_copy(2).wait_send()

    for n in range(1, 3):
        a_copy(n).wait_send()
    p_copy().wait_send()
    for n in range(2):
        d_copy(n).wait_send()
    for r in range(rhs):
        for i in range(2):
            in_copy(r, i).wait_send()
    q_copy().wait_send()
    q_copy(True).wait_recv()
    for n in range(len(PIECES)):
        f_copy(n).wait_send()
        for i in range(2):
            y_copy(n, i).wait_send()
            y_copy(n, i, True).wait_recv()


def solution(mesh):
    def local(w, x):
        rhs, rows, cols = x.shape
        sems = []
        for shape in ((3,), (rhs, 2), (2,), (len(PIECES),), (1,), (len(PIECES), 2), (1,)):
            sems += [pltpu.SemaphoreType.DMA(shape)] * 2
        return pl.pallas_call(
            kernel,
            out_shape=pltpu.VMEM(x.shape, x.dtype),
            in_specs=[pl.BlockSpec(memory_space=pl.ANY)] * 2,
            out_specs=pl.BlockSpec(memory_space=pltpu.VMEM),
            scratch_shapes=[
                pltpu.VMEM((2, 2, rows, w.shape[1] * 2), w.dtype),
                pltpu.VMEM((rhs, 2, 2, 2, rows, cols // SIDE), x.dtype),
                pltpu.VMEM((rhs, SIDE * rows, cols // SIDE), x.dtype),
                *sems,
                pltpu.SemaphoreType.DMA((2,)),
                pltpu.SemaphoreType.REGULAR,
                pltpu.VMEM((2, MOVED, w.shape[1]), w.dtype),
                pltpu.SemaphoreType.DMA((3,)),
                pltpu.SemaphoreType.DMA((3,)),
            ],
            compiler_params=pltpu.CompilerParams(collective_id=0, has_side_effects=True, vmem_limit_bytes=52 * 1024 * 1024),
        )(w, x)

    return jax.shard_map(local, mesh=mesh, in_specs=(P(("row", "depth"), "col"), P(None, ("row", "depth"), "col")),
                         out_specs=P(None, ("row", "depth"), "col"), check_vma=False)
```

```python
import functools

import jax
import jax.numpy as jnp
from jax import lax
from jax.experimental import pallas as pl
from jax.experimental.pallas import tpu as pltpu
from jax.sharding import PartitionSpec as P

MESH = pl.DeviceIdType.MESH
SIDE = 4
PIECES = ((0, 0, 1024), (1, 0, 1024), (2, 0, 512), (2, 512, 256), (2, 768, 256))
SPLIT = 2
WIDE = 256
MOVED = 16


def kernel(w_ref, x_ref, y_ref, a_buf, x_buf, y_buf, a_send, a_recv, in_send, in_recv, d_send, d_recv, f_send, f_recv,
           p_send, p_recv, y_send, y_recv, q_send, q_recv, own_sem, ready, e_buf, g_buf, e_send, e_recv):
    z, j, row = lax.axis_index("depth"), lax.axis_index("col"), lax.axis_index("row")
    x, c = row // 2, row % 2
    rhs, rows, cols = x_ref.shape
    kcols = w_ref.shape[1]
    group = cols // SIDE

    def peer(k):
        kz, kc, kx = k // 4 % 2, k // 2 % 2, k % 2
        return x + kx * (1 - 2 * x), c + kc * (1 - 2 * c), z + kz * (1 - 2 * z)

    def device(k):
        px, pc, pz = peer(k)
        return (pz, j, px * 2 + pc)

    def in_side(k):
        px, pc, _ = peer(k)
        return pc * 2 + px

    other_y = (z, 1 - j, row)

    def remote(src, dst, send, recv, to):
        return pltpu.make_async_remote_copy(src, dst, send, recv, device_id=to, device_id_type=MESH)

    def a_block(k, jj):
        px, pc, _ = peer(k)
        return a_buf.at[pc, px, :, pl.ds(pl.multiple_of(jj * kcols, kcols), kcols)]

    def rows_of(k):
        return pl.ds(pl.multiple_of(in_side(k) * rows, rows), rows)

    def a_copy(n, receive=False):
        if n == 0:
            src, here, to = w_ref, a_block(1, j), device(1)
            there = a_block(0, j)
        elif n == 1:
            there, here = (a_buf.at[c, :, :, pl.ds(pl.multiple_of(jj * kcols, kcols), kcols)] for jj in (j, 1 - j))
            src, to = there, other_y
        else:
            there, here = a_buf.at[c], a_buf.at[1 - c]
            src, to = there, device(2)
        return remote(src, here if receive else there, a_send.at[n], a_recv.at[n], to)

    half = kcols // 2
    last = pl.ds(rows - MOVED, MOVED)

    def a_over_x(side, op):
        low = (j == 0) & (z == 0) & (c == 0)
        high = (z == 0) & (x == side) & (c == 0)

        def some(cut_low, cut_high):
            at = pl.ds(MOVED * cut_low, rows - MOVED * (cut_low + cut_high))

            def copy(receive=False):
                dst = a_block(1 if receive else 0, j).at[at, :]
                return remote(w_ref.at[at, :], dst, a_send.at[0], a_recv.at[0], device(1))

            has_low = low if cut_low else jnp.logical_not(low)
            has_high = high if cut_high else jnp.logical_not(high)
            pl.when(has_low & has_high)(lambda: op(copy))

        for cut_low in range(2):
            for cut_high in range(2):
                some(cut_low, cut_high)

        @pl.when(high)
        def _():
            at = (last, pl.ds(half, half))

            def copy(receive=False):
                dst = a_block(1 if receive else 0, j).at[at]
                return remote(w_ref.at[at], dst, e_send.at[3], e_recv.at[3], device(1))

            op(copy)

    def g_copy(n):
        at = (last, pl.ds(0, half))
        src, there, to = (
            (w_ref.at[at], g_buf.at[0], device(4)),
            (g_buf.at[0], g_buf.at[1], device(1)),
            (g_buf.at[1], a_block(1, j).at[at], device(4)),
        )[n]
        return remote(src, there, e_send.at[4 + n], e_recv.at[4 + n], to)

    def when_at(px, pz, body):
        pl.when((x == px) & (z == pz) & (c == 0))(body)

    def e_copy(n, receive=False):
        if n == 0:
            src, there, to = w_ref.at[pl.ds(0, MOVED), :], e_buf.at[0], other_y
        elif n == 1:
            src, there, to = e_buf.at[0], e_buf.at[1], device(1)
        else:
            src, there, to = e_buf.at[1], a_block(1, 0).at[pl.ds(0, MOVED), :], other_y
        return remote(src, there, e_send.at[n], e_recv.at[n], to)

    def when_moved(plane, body):
        pl.when((j == plane) & (z == 0) & (c == 0))(body)

    def given(piece, k):
        r, at, width = piece
        return (r, slice(None), pl.ds(pl.multiple_of(in_side(k) * group + at, WIDE), width))

    def held(piece, k):
        r, at, width = piece
        px, pc, pz = peer(k)
        return x_buf.at[r, px, pc, pz, :, pl.ds(at, width)]

    def x_copy(piece, k, send, recv, receive=False):
        return remote(x_ref.at[given(piece, k)], held(piece, k if receive else 0), send, recv, device(k))

    def in_copy(r, i, receive=False):
        return x_copy((r, 0, group), (1, 3)[i], in_send.at[r, i], in_recv.at[r, i], receive)

    def onward(piece, side, send, recv, receive):
        r, at, width = piece
        src, here = (x_buf.at[r, side, :, pz, :, pl.ds(at, width)] for pz in (z, 1 - z))
        return remote(src, here if receive else src, send, recv, device(4))

    ahead = (pl.ds(0, SPLIT), 0, group)

    def d_copy(n, receive=False):
        if n == 0:
            return x_copy(ahead, 4, d_send.at[n], d_recv.at[n], receive)
        src, here = (x_buf.at[ahead[0], x, 1 - c, pz] for pz in (z, 1 - z))
        return remote(src, here if receive else src, d_send.at[n], d_recv.at[n], device(4))

    def f_copy(n, receive=False):
        side = 1 - x if PIECES[n][0] < SPLIT else slice(None)
        return onward(PIECES[n], side, f_send.at[n], f_recv.at[n], receive)

    everything = (slice(None), 0, group)

    def p_copy(receive=False):
        return x_copy(everything, 2, p_send.at[0], p_recv.at[0], receive)

    def y_copy(n, kc, receive=False):
        k = kc * 2 + 1
        r, at, width = PIECES[n]
        src = y_buf.at[r, rows_of(k), pl.ds(at, width)]
        return remote(src, y_ref.at[given(PIECES[n], k if receive else 0)], y_send.at[n, kc], y_recv.at[n, kc], device(k))

    def q_copy(receive=False):
        there = y_ref.at[given(everything, 2 if receive else 0)]
        return remote(y_buf.at[:, rows_of(2), :], there, q_send.at[0], q_recv.at[0], device(2))

    own_a = pltpu.make_async_copy(w_ref, a_block(0, j), own_sem.at[0])
    own_x = pltpu.make_async_copy(x_ref.at[given(everything, 0)], held(everything, 0), own_sem.at[1])

    def product(k, r, at):
        xs = x_buf[r, :, :, :, :, pl.ds(at, WIDE)].reshape(-1, WIDE)
        return jnp.dot(a_buf[peer(k)[1], peer(k)[0]], xs, preferred_element_type=jnp.float32).astype(y_buf.dtype)

    def forward(n):
        r, at, _ = PIECES[n]
        if at == 0:
            for i in range(2):
                in_copy(r, i, True).wait_recv()
        f_copy(n).start()

    def multiply(n):
        r, at, width = PIECES[n]
        if n == 0:
            for m in range(2):
                d_copy(m, True).wait_recv()
        f_copy(n, True).wait_recv()
        parts = width // WIDE

        def tile(s, carry):
            t, at_s = s // parts, at + s % parts * WIDE
            kz = 1 - t // 2
            k = (t % 2 + t // 2) % 2 * 2 + kz
            at_s = pl.multiple_of(at_s, WIDE)
            y_buf[r, rows_of(k), pl.ds(at_s, WIDE)] = product(k, r, at_s)

            @pl.when(s % parts == 0)
            def _():
                for i in range(2):
                    @pl.when(t == i + 1)
                    def _():
                        y_copy(n, i).start()

            return carry

        lax.fori_loop(0, 3 * parts, tile, 0)

        def own(s, carry):
            at_s = pl.multiple_of(at + s * WIDE, WIDE)
            y_ref[r, :, pl.ds(pl.multiple_of(in_side(0) * group + at_s, WIDE), WIDE)] = product(0, r, at_s)
            return carry

        lax.fori_loop(0, parts, own, 0)

    barrier = pltpu.get_barrier_semaphore()
    pl.semaphore_signal(barrier, inc=1, device_id=device(1), device_id_type=MESH)
    beside = (device(4), other_y, device(2))
    own_x.start()
    own_a.start()

    @pl.when(x == 0)
    def _():
        for to in beside:
            pl.semaphore_signal(barrier, inc=1, device_id=to, device_id_type=MESH)
        pl.semaphore_wait(barrier, 4)
        for to in beside:
            pl.semaphore_signal(ready, inc=1, device_id=to, device_id_type=MESH)

    @pl.when(x == 1)
    def _():
        pl.semaphore_wait(barrier, 1)

    def other_links():
        when_at(0, 0, lambda: g_copy(0).start())
        d_copy(0).start()
        p_copy().start()

    a_over_x(0, lambda copy: copy().start())
    pl.when(x == 0)(other_links)

    @pl.when(x == 0)
    def _():
        pl.semaphore_wait(ready, 3)
        pl.semaphore_signal(ready, inc=1, device_id=device(1), device_id_type=MESH)

    @pl.when(x == 1)
    def _():
        pl.semaphore_wait(ready, 1)
        other_links()

    when_moved(0, lambda: e_copy(0).start())

    @functools.partial(when_moved, 1)
    def _():
        e_copy(0, True).wait_recv()
        e_copy(1).start()

    @functools.partial(when_at, 0, 1)
    def _():
        g_copy(0).wait_recv()
        g_copy(1).start()

    for r in range(rhs):
        for i in range(2):
            in_copy(r, i).start()
    own_x.wait()
    p_copy(True).wait_recv()

    @functools.partial(when_at, 1, 1)
    def _():
        g_copy(1).wait_recv()
        g_copy(2).start()

    d_copy(1).start()
    own_a.wait()
    a_over_x(1, lambda copy: copy(True).wait_recv())

    @functools.partial(when_moved, 1)
    def _():
        e_copy(1, True).wait_recv()
        e_copy(2).start()

    when_moved(0, lambda: e_copy(2, True).wait_recv())
    when_at(1, 0, lambda: g_copy(2).wait_recv())
    a_copy(1).start()
    forward(0)
    a_copy(1, True).wait_recv()
    a_copy(2).start()
    a_copy(2, True).wait_recv()
    forward(1)
    multiply(0)
    forward(2)
    multiply(1)
    forward(3)
    forward(4)
    for n in range(2, len(PIECES)):
        multiply(n)

    q_copy().start()
    a_over_x(0, lambda copy: copy().wait_send())
    when_at(0, 0, lambda: g_copy(0).wait_send())
    when_at(0, 1, lambda: g_copy(1).wait_send())
    when_at(1, 1, lambda: g_copy(2).wait_send())
    when_moved(0, lambda: e_copy(0).wait_send())

    @functools.partial(when_moved, 1)
    def _():
        e_copy(1).wait_send()
        e_copy(2).wait_send()

    for n in range(1, 3):
        a_copy(n).wait_send()
    p_copy().wait_send()
    for n in range(2):
        d_copy(n).wait_send()
    for r in range(rhs):
        for i in range(2):
            in_copy(r, i).wait_send()
    q_copy().wait_send()
    q_copy(True).wait_recv()
    for n in range(len(PIECES)):
        f_copy(n).wait_send()
        for i in range(2):
            y_copy(n, i).wait_send()
            y_copy(n, i, True).wait_recv()


def solution(mesh):
    def local(w, x):
        rhs, rows, cols = x.shape
        sems = []
        for shape in ((3,), (rhs, 2), (2,), (len(PIECES),), (1,), (len(PIECES), 2), (1,)):
            sems += [pltpu.SemaphoreType.DMA(shape)] * 2
        return pl.pallas_call(
            kernel,
            out_shape=pltpu.VMEM(x.shape, x.dtype),
            in_specs=[pl.BlockSpec(memory_space=pl.ANY)] * 2,
            out_specs=pl.BlockSpec(memory_space=pltpu.VMEM),
            scratch_shapes=[
                pltpu.VMEM((2, 2, rows, w.shape[1] * 2), w.dtype),
                pltpu.VMEM((rhs, 2, 2, 2, rows, cols // SIDE), x.dtype),
                pltpu.VMEM((rhs, SIDE * rows, cols // SIDE), x.dtype),
                *sems,
                pltpu.SemaphoreType.DMA((2,)),
                pltpu.SemaphoreType.REGULAR,
                pltpu.VMEM((2, MOVED, w.shape[1]), w.dtype),
                pltpu.VMEM((2, MOVED, w.shape[1] // 2), w.dtype),
                pltpu.SemaphoreType.DMA((7,)),
                pltpu.SemaphoreType.DMA((7,)),
            ],
            compiler_params=pltpu.CompilerParams(collective_id=0, has_side_effects=True, vmem_limit_bytes=52 * 1024 * 1024),
        )(w, x)

    return jax.shard_map(local, mesh=mesh, in_specs=(P(("row", "depth"), "col"), P(None, ("row", "depth"), "col")),
                         out_specs=P(None, ("row", "depth"), "col"), check_vma=False)
```

```python
import functools

import jax
import jax.numpy as jnp
from jax import lax
from jax.experimental import pallas as pl
from jax.experimental.pallas import tpu as pltpu
from jax.sharding import PartitionSpec as P

MESH = pl.DeviceIdType.MESH
SIDE = 4
PIECES = ((0, 0, 1024), (1, 0, 1024), (2, 0, 512), (2, 512, 256), (2, 768, 256))
SPLIT = 2
WIDE = 256
MOVED = 16


def kernel(w_ref, x_ref, y_ref, a_buf, x_buf, y_buf, a_send, a_recv, in_send, in_recv, d_send, d_recv, f_send, f_recv,
           p_send, p_recv, y_send, y_recv, q_send, q_recv, own_sem, ready, e_buf, g_buf, e_send, e_recv):
    z, j, row = lax.axis_index("depth"), lax.axis_index("col"), lax.axis_index("row")
    x, c = row // 2, row % 2
    rhs, rows, cols = x_ref.shape
    kcols = w_ref.shape[1]
    group = cols // SIDE

    def peer(k):
        kz, kc, kx = k // 4 % 2, k // 2 % 2, k % 2
        return x + kx * (1 - 2 * x), c + kc * (1 - 2 * c), z + kz * (1 - 2 * z)

    def device(k):
        px, pc, pz = peer(k)
        return (pz, j, px * 2 + pc)

    def in_side(k):
        px, pc, _ = peer(k)
        return pc * 2 + px

    other_y = (z, 1 - j, row)

    def remote(src, dst, send, recv, to):
        return pltpu.make_async_remote_copy(src, dst, send, recv, device_id=to, device_id_type=MESH)

    def a_block(k, jj):
        px, pc, _ = peer(k)
        return a_buf.at[pc, px, :, pl.ds(pl.multiple_of(jj * kcols, kcols), kcols)]

    def rows_of(k):
        return pl.ds(pl.multiple_of(in_side(k) * rows, rows), rows)

    def a_copy(n, receive=False):
        if n == 0:
            src, here, to = w_ref, a_block(1, j), device(1)
            there = a_block(0, j)
        elif n == 1:
            there, here = (a_buf.at[c, :, :, pl.ds(pl.multiple_of(jj * kcols, kcols), kcols)] for jj in (j, 1 - j))
            src, to = there, other_y
        else:
            there, here = a_buf.at[c], a_buf.at[1 - c]
            src, to = there, device(2)
        return remote(src, here if receive else there, a_send.at[n], a_recv.at[n], to)

    few = MOVED // 2
    last = pl.ds(rows - few, few)

    def a_over_x(side, op):
        low = (j == 0) & (z == 0) & (c == 0)
        high = (z == 0) & (x == side) & (c == 0)

        def some(cut_low, cut_high):
            at = pl.ds(MOVED * cut_low, rows - MOVED * cut_low - few * cut_high)

            def copy(receive=False):
                dst = a_block(1 if receive else 0, j).at[at, :]
                return remote(w_ref.at[at, :], dst, a_send.at[0], a_recv.at[0], device(1))

            has_low = low if cut_low else jnp.logical_not(low)
            has_high = high if cut_high else jnp.logical_not(high)
            pl.when(has_low & has_high)(lambda: op(copy))

        for cut_low in range(2):
            for cut_high in range(2):
                some(cut_low, cut_high)

    def g_copy(n):
        at = (last, slice(None))
        src, there, to = (
            (w_ref.at[at], g_buf.at[0], device(4)),
            (g_buf.at[0], g_buf.at[1], device(1)),
            (g_buf.at[1], a_block(1, j).at[at], device(4)),
        )[n]
        return remote(src, there, e_send.at[3 + n], e_recv.at[3 + n], to)

    def when_at(px, pz, body):
        pl.when((x == px) & (z == pz) & (c == 0))(body)

    def e_copy(n, receive=False):
        if n == 0:
            src, there, to = w_ref.at[pl.ds(0, MOVED), :], e_buf.at[0], other_y
        elif n == 1:
            src, there, to = e_buf.at[0], e_buf.at[1], device(1)
        else:
            src, there, to = e_buf.at[1], a_block(1, 0).at[pl.ds(0, MOVED), :], other_y
        return remote(src, there, e_send.at[n], e_recv.at[n], to)

    def when_moved(plane, body):
        pl.when((j == plane) & (z == 0) & (c == 0))(body)

    def given(piece, k):
        r, at, width = piece
        return (r, slice(None), pl.ds(pl.multiple_of(in_side(k) * group + at, WIDE), width))

    def held(piece, k):
        r, at, width = piece
        px, pc, pz = peer(k)
        return x_buf.at[r, px, pc, pz, :, pl.ds(at, width)]

    def x_copy(piece, k, send, recv, receive=False):
        return remote(x_ref.at[given(piece, k)], held(piece, k if receive else 0), send, recv, device(k))

    def in_copy(r, i, receive=False):
        return x_copy((r, 0, group), (1, 3)[i], in_send.at[r, i], in_recv.at[r, i], receive)

    def onward(piece, side, send, recv, receive):
        r, at, width = piece
        src, here = (x_buf.at[r, side, :, pz, :, pl.ds(at, width)] for pz in (z, 1 - z))
        return remote(src, here if receive else src, send, recv, device(4))

    ahead = (pl.ds(0, SPLIT), 0, group)

    def d_copy(n, receive=False):
        if n == 0:
            return x_copy(ahead, 4, d_send.at[n], d_recv.at[n], receive)
        src, here = (x_buf.at[ahead[0], x, 1 - c, pz] for pz in (z, 1 - z))
        return remote(src, here if receive else src, d_send.at[n], d_recv.at[n], device(4))

    def f_copy(n, receive=False):
        side = 1 - x if PIECES[n][0] < SPLIT else slice(None)
        return onward(PIECES[n], side, f_send.at[n], f_recv.at[n], receive)

    everything = (slice(None), 0, group)

    def p_copy(receive=False):
        return x_copy(everything, 2, p_send.at[0], p_recv.at[0], receive)

    def y_copy(n, kc, receive=False):
        k = kc * 2 + 1
        r, at, width = PIECES[n]
        src = y_buf.at[r, rows_of(k), pl.ds(at, width)]
        return remote(src, y_ref.at[given(PIECES[n], k if receive else 0)], y_send.at[n, kc], y_recv.at[n, kc], device(k))

    def q_copy(receive=False):
        there = y_ref.at[given(everything, 2 if receive else 0)]
        return remote(y_buf.at[:, rows_of(2), :], there, q_send.at[0], q_recv.at[0], device(2))

    own_a = pltpu.make_async_copy(w_ref, a_block(0, j), own_sem.at[0])
    own_x = pltpu.make_async_copy(x_ref.at[given(everything, 0)], held(everything, 0), own_sem.at[1])

    def product(k, r, at):
        xs = x_buf[r, :, :, :, :, pl.ds(at, WIDE)].reshape(-1, WIDE)
        return jnp.dot(a_buf[peer(k)[1], peer(k)[0]], xs, preferred_element_type=jnp.float32).astype(y_buf.dtype)

    def forward(n):
        r, at, _ = PIECES[n]
        if at == 0:
            for i in range(2):
                in_copy(r, i, True).wait_recv()
        f_copy(n).start()

    def multiply(n):
        r, at, width = PIECES[n]
        if n == 0:
            for m in range(2):
                d_copy(m, True).wait_recv()
        f_copy(n, True).wait_recv()
        parts = width // WIDE

        def tile(s, carry):
            t, at_s = s // parts, at + s % parts * WIDE
            kz = 1 - t // 2
            k = (t % 2 + t // 2) % 2 * 2 + kz
            at_s = pl.multiple_of(at_s, WIDE)
            y_buf[r, rows_of(k), pl.ds(at_s, WIDE)] = product(k, r, at_s)

            @pl.when(s % parts == 0)
            def _():
                for i in range(2):
                    @pl.when(t == i + 1)
                    def _():
                        y_copy(n, i).start()

            return carry

        lax.fori_loop(0, 3 * parts, tile, 0)

        def own(s, carry):
            at_s = pl.multiple_of(at + s * WIDE, WIDE)
            y_ref[r, :, pl.ds(pl.multiple_of(in_side(0) * group + at_s, WIDE), WIDE)] = product(0, r, at_s)
            return carry

        lax.fori_loop(0, parts, own, 0)

    barrier = pltpu.get_barrier_semaphore()
    pl.semaphore_signal(barrier, inc=1, device_id=device(1), device_id_type=MESH)
    beside = (device(4), other_y, device(2))
    own_x.start()
    own_a.start()

    @pl.when(x == 0)
    def _():
        for to in beside:
            pl.semaphore_signal(barrier, inc=1, device_id=to, device_id_type=MESH)
        pl.semaphore_wait(barrier, 4)
        for to in beside:
            pl.semaphore_signal(ready, inc=1, device_id=to, device_id_type=MESH)

    @pl.when(x == 1)
    def _():
        pl.semaphore_wait(barrier, 1)

    def other_links():
        when_at(0, 0, lambda: g_copy(0).start())
        d_copy(0).start()
        p_copy().start()

    a_over_x(0, lambda copy: copy().start())
    pl.when(x == 0)(other_links)

    @pl.when(x == 0)
    def _():
        pl.semaphore_wait(ready, 3)
        pl.semaphore_signal(ready, inc=1, device_id=device(1), device_id_type=MESH)

    @pl.when(x == 1)
    def _():
        pl.semaphore_wait(ready, 1)
        other_links()

    when_moved(0, lambda: e_copy(0).start())

    @functools.partial(when_moved, 1)
    def _():
        e_copy(0, True).wait_recv()
        e_copy(1).start()

    @functools.partial(when_at, 0, 1)
    def _():
        g_copy(0).wait_recv()
        g_copy(1).start()

    for r in range(rhs):
        for i in range(2):
            in_copy(r, i).start()
    own_x.wait()
    p_copy(True).wait_recv()

    @functools.partial(when_at, 1, 1)
    def _():
        g_copy(1).wait_recv()
        g_copy(2).start()

    d_copy(1).start()
    own_a.wait()
    a_over_x(1, lambda copy: copy(True).wait_recv())

    @functools.partial(when_moved, 1)
    def _():
        e_copy(1, True).wait_recv()
        e_copy(2).start()

    when_moved(0, lambda: e_copy(2, True).wait_recv())
    when_at(1, 0, lambda: g_copy(2).wait_recv())
    a_copy(1).start()
    forward(0)
    a_copy(1, True).wait_recv()
    a_copy(2).start()
    a_copy(2, True).wait_recv()
    forward(1)
    multiply(0)
    forward(2)
    multiply(1)
    forward(3)
    forward(4)
    for n in range(2, len(PIECES)):
        multiply(n)

    q_copy().start()
    a_over_x(0, lambda copy: copy().wait_send())
    when_at(0, 0, lambda: g_copy(0).wait_send())
    when_at(0, 1, lambda: g_copy(1).wait_send())
    when_at(1, 1, lambda: g_copy(2).wait_send())
    when_moved(0, lambda: e_copy(0).wait_send())

    @functools.partial(when_moved, 1)
    def _():
        e_copy(1).wait_send()
        e_copy(2).wait_send()

    for n in range(1, 3):
        a_copy(n).wait_send()
    p_copy().wait_send()
    for n in range(2):
        d_copy(n).wait_send()
    for r in range(rhs):
        for i in range(2):
            in_copy(r, i).wait_send()
    q_copy().wait_send()
    q_copy(True).wait_recv()
    for n in range(len(PIECES)):
        f_copy(n).wait_send()
        for i in range(2):
            y_copy(n, i).wait_send()
            y_copy(n, i, True).wait_recv()


def solution(mesh):
    def local(w, x):
        rhs, rows, cols = x.shape
        sems = []
        for shape in ((3,), (rhs, 2), (2,), (len(PIECES),), (1,), (len(PIECES), 2), (1,)):
            sems += [pltpu.SemaphoreType.DMA(shape)] * 2
        return pl.pallas_call(
            kernel,
            out_shape=pltpu.VMEM(x.shape, x.dtype),
            in_specs=[pl.BlockSpec(memory_space=pl.ANY)] * 2,
            out_specs=pl.BlockSpec(memory_space=pltpu.VMEM),
            scratch_shapes=[
                pltpu.VMEM((2, 2, rows, w.shape[1] * 2), w.dtype),
                pltpu.VMEM((rhs, 2, 2, 2, rows, cols // SIDE), x.dtype),
                pltpu.VMEM((rhs, SIDE * rows, cols // SIDE), x.dtype),
                *sems,
                pltpu.SemaphoreType.DMA((2,)),
                pltpu.SemaphoreType.REGULAR,
                pltpu.VMEM((2, MOVED, w.shape[1]), w.dtype),
                pltpu.VMEM((2, MOVED // 2, w.shape[1]), w.dtype),
                pltpu.SemaphoreType.DMA((6,)),
                pltpu.SemaphoreType.DMA((6,)),
            ],
            compiler_params=pltpu.CompilerParams(collective_id=0, has_side_effects=True, vmem_limit_bytes=52 * 1024 * 1024),
        )(w, x)

    return jax.shard_map(local, mesh=mesh, in_specs=(P(("row", "depth"), "col"), P(None, ("row", "depth"), "col")),
                         out_specs=P(None, ("row", "depth"), "col"), check_vma=False)
```

```python
import functools

import jax
import jax.numpy as jnp
from jax import lax
from jax.experimental import pallas as pl
from jax.experimental.pallas import tpu as pltpu
from jax.sharding import PartitionSpec as P

MESH = pl.DeviceIdType.MESH
SIDE = 4
PIECES = ((0, 0, 1024), (1, 0, 1024), (2, 0, 512), (2, 512, 256), (2, 768, 256))
SPLIT = 2
WIDE = 256
MOVED = 16


def kernel(w_ref, x_ref, y_ref, a_buf, x_buf, y_buf, a_send, a_recv, in_send, in_recv, d_send, d_recv, f_send, f_recv,
           p_send, p_recv, y_send, y_recv, q_send, q_recv, own_sem, ready, e_buf, g_buf, e_send, e_recv):
    z, j, row = lax.axis_index("depth"), lax.axis_index("col"), lax.axis_index("row")
    x, c = row // 2, row % 2
    rhs, rows, cols = x_ref.shape
    kcols = w_ref.shape[1]
    group = cols // SIDE

    def peer(k):
        kz, kc, kx = k // 4 % 2, k // 2 % 2, k % 2
        return x + kx * (1 - 2 * x), c + kc * (1 - 2 * c), z + kz * (1 - 2 * z)

    def device(k):
        px, pc, pz = peer(k)
        return (pz, j, px * 2 + pc)

    def in_side(k):
        px, pc, _ = peer(k)
        return pc * 2 + px

    other_y = (z, 1 - j, row)

    def remote(src, dst, send, recv, to):
        return pltpu.make_async_remote_copy(src, dst, send, recv, device_id=to, device_id_type=MESH)

    def a_block(k, jj):
        px, pc, _ = peer(k)
        return a_buf.at[pc, px, :, pl.ds(pl.multiple_of(jj * kcols, kcols), kcols)]

    def rows_of(k):
        return pl.ds(pl.multiple_of(in_side(k) * rows, rows), rows)

    def a_copy(n, receive=False):
        if n == 0:
            src, here, to = w_ref, a_block(1, j), device(1)
            there = a_block(0, j)
        elif n == 1:
            there, here = (a_buf.at[c, :, :, pl.ds(pl.multiple_of(jj * kcols, kcols), kcols)] for jj in (j, 1 - j))
            src, to = there, other_y
        else:
            there, here = a_buf.at[c], a_buf.at[1 - c]
            src, to = there, device(2)
        return remote(src, here if receive else there, a_send.at[n], a_recv.at[n], to)

    few = MOVED // 2
    last = pl.ds(rows - few, few)

    def a_over_x(op):
        low = (j == 0) & (z == 0) & (c == 0)
        high = (z == 0) & (c == 0)

        def some(cut_low, cut_high):
            at = pl.ds(MOVED * cut_low, rows - MOVED * cut_low - few * cut_high)

            def copy(receive=False):
                dst = a_block(1 if receive else 0, j).at[at, :]
                return remote(w_ref.at[at, :], dst, a_send.at[0], a_recv.at[0], device(1))

            has_low = low if cut_low else jnp.logical_not(low)
            has_high = high if cut_high else jnp.logical_not(high)
            pl.when(has_low & has_high)(lambda: op(copy))

        for cut_low in range(2):
            for cut_high in range(2):
                some(cut_low, cut_high)

    def g_copy(n):
        at = (last, slice(None))
        src, there, to = (
            (w_ref.at[at], g_buf.at[0], device(4)),
            (g_buf.at[0], g_buf.at[1], device(1)),
            (g_buf.at[1], a_block(1, j).at[at], device(4)),
        )[n]
        return remote(src, there, e_send.at[3 + n], e_recv.at[3 + n], to)

    def when_at(pz, body):
        pl.when((z == pz) & (c == 0))(body)

    def e_copy(n, receive=False):
        if n == 0:
            src, there, to = w_ref.at[pl.ds(0, MOVED), :], e_buf.at[0], other_y
        elif n == 1:
            src, there, to = e_buf.at[0], e_buf.at[1], device(1)
        else:
            src, there, to = e_buf.at[1], a_block(1, 0).at[pl.ds(0, MOVED), :], other_y
        return remote(src, there, e_send.at[n], e_recv.at[n], to)

    def when_moved(plane, body):
        pl.when((j == plane) & (z == 0) & (c == 0))(body)

    def given(piece, k):
        r, at, width = piece
        return (r, slice(None), pl.ds(pl.multiple_of(in_side(k) * group + at, WIDE), width))

    def held(piece, k):
        r, at, width = piece
        px, pc, pz = peer(k)
        return x_buf.at[r, px, pc, pz, :, pl.ds(at, width)]

    def x_copy(piece, k, send, recv, receive=False):
        return remote(x_ref.at[given(piece, k)], held(piece, k if receive else 0), send, recv, device(k))

    def in_copy(r, i, receive=False):
        return x_copy((r, 0, group), (1, 3)[i], in_send.at[r, i], in_recv.at[r, i], receive)

    def onward(piece, side, send, recv, receive):
        r, at, width = piece
        src, here = (x_buf.at[r, side, :, pz, :, pl.ds(at, width)] for pz in (z, 1 - z))
        return remote(src, here if receive else src, send, recv, device(4))

    ahead = (pl.ds(0, SPLIT), 0, group)

    def d_copy(n, receive=False):
        if n == 0:
            return x_copy(ahead, 4, d_send.at[n], d_recv.at[n], receive)
        src, here = (x_buf.at[ahead[0], x, 1 - c, pz] for pz in (z, 1 - z))
        return remote(src, here if receive else src, d_send.at[n], d_recv.at[n], device(4))

    def f_copy(n, receive=False):
        side = 1 - x if PIECES[n][0] < SPLIT else slice(None)
        return onward(PIECES[n], side, f_send.at[n], f_recv.at[n], receive)

    everything = (slice(None), 0, group)

    def p_copy(receive=False):
        return x_copy(everything, 2, p_send.at[0], p_recv.at[0], receive)

    def y_copy(n, kc, receive=False):
        k = kc * 2 + 1
        r, at, width = PIECES[n]
        src = y_buf.at[r, rows_of(k), pl.ds(at, width)]
        return remote(src, y_ref.at[given(PIECES[n], k if receive else 0)], y_send.at[n, kc], y_recv.at[n, kc], device(k))

    def q_copy(receive=False):
        there = y_ref.at[given(everything, 2 if receive else 0)]
        return remote(y_buf.at[:, rows_of(2), :], there, q_send.at[0], q_recv.at[0], device(2))

    own_a = pltpu.make_async_copy(w_ref, a_block(0, j), own_sem.at[0])
    own_x = pltpu.make_async_copy(x_ref.at[given(everything, 0)], held(everything, 0), own_sem.at[1])

    def product(k, r, at):
        xs = x_buf[r, :, :, :, :, pl.ds(at, WIDE)].reshape(-1, WIDE)
        return jnp.dot(a_buf[peer(k)[1], peer(k)[0]], xs, preferred_element_type=jnp.float32).astype(y_buf.dtype)

    def forward(n):
        r, at, _ = PIECES[n]
        if at == 0:
            for i in range(2):
                in_copy(r, i, True).wait_recv()
        f_copy(n).start()

    def multiply(n):
        r, at, width = PIECES[n]
        if n == 0:
            for m in range(2):
                d_copy(m, True).wait_recv()
        f_copy(n, True).wait_recv()
        parts = width // WIDE

        def tile(s, carry):
            t, at_s = s // parts, at + s % parts * WIDE
            kz = 1 - t // 2
            k = (t % 2 + t // 2) % 2 * 2 + kz
            at_s = pl.multiple_of(at_s, WIDE)
            y_buf[r, rows_of(k), pl.ds(at_s, WIDE)] = product(k, r, at_s)

            @pl.when(s % parts == 0)
            def _():
                for i in range(2):
                    @pl.when(t == i + 1)
                    def _():
                        y_copy(n, i).start()

            return carry

        lax.fori_loop(0, 3 * parts, tile, 0)

        def own(s, carry):
            at_s = pl.multiple_of(at + s * WIDE, WIDE)
            y_ref[r, :, pl.ds(pl.multiple_of(in_side(0) * group + at_s, WIDE), WIDE)] = product(0, r, at_s)
            return carry

        lax.fori_loop(0, parts, own, 0)

    barrier = pltpu.get_barrier_semaphore()
    pl.semaphore_signal(barrier, inc=1, device_id=device(1), device_id_type=MESH)
    beside = (device(4), other_y, device(2))
    own_x.start()
    own_a.start()

    @pl.when(x == 0)
    def _():
        for to in beside:
            pl.semaphore_signal(barrier, inc=1, device_id=to, device_id_type=MESH)
        pl.semaphore_wait(barrier, 4)
        for to in beside:
            pl.semaphore_signal(ready, inc=1, device_id=to, device_id_type=MESH)

    @pl.when(x == 1)
    def _():
        pl.semaphore_wait(barrier, 1)

    def other_links():
        when_at(0, lambda: g_copy(0).start())
        d_copy(0).start()
        p_copy().start()

    a_over_x(lambda copy: copy().start())
    pl.when(x == 0)(other_links)

    @pl.when(x == 0)
    def _():
        pl.semaphore_wait(ready, 3)
        pl.semaphore_signal(ready, inc=1, device_id=device(1), device_id_type=MESH)

    @pl.when(x == 1)
    def _():
        pl.semaphore_wait(ready, 1)
        other_links()

    when_moved(0, lambda: e_copy(0).start())

    @functools.partial(when_moved, 1)
    def _():
        e_copy(0, True).wait_recv()
        e_copy(1).start()

    @functools.partial(when_at, 1)
    def _():
        g_copy(0).wait_recv()
        g_copy(1).start()

    for r in range(rhs):
        for i in range(2):
            in_copy(r, i).start()
    own_x.wait()
    p_copy(True).wait_recv()

    @functools.partial(when_at, 1)
    def _():
        g_copy(1).wait_recv()
        g_copy(2).start()

    d_copy(1).start()
    own_a.wait()
    a_over_x(lambda copy: copy(True).wait_recv())

    @functools.partial(when_moved, 1)
    def _():
        e_copy(1, True).wait_recv()
        e_copy(2).start()

    when_moved(0, lambda: e_copy(2, True).wait_recv())
    when_at(0, lambda: g_copy(2).wait_recv())
    a_copy(1).start()
    forward(0)
    a_copy(1, True).wait_recv()
    a_copy(2).start()
    a_copy(2, True).wait_recv()
    forward(1)
    multiply(0)
    forward(2)
    multiply(1)
    forward(3)
    forward(4)
    for n in range(2, len(PIECES)):
        multiply(n)

    q_copy().start()
    a_over_x(lambda copy: copy().wait_send())
    when_at(0, lambda: g_copy(0).wait_send())
    when_at(1, lambda: g_copy(1).wait_send())
    when_at(1, lambda: g_copy(2).wait_send())
    when_moved(0, lambda: e_copy(0).wait_send())

    @functools.partial(when_moved, 1)
    def _():
        e_copy(1).wait_send()
        e_copy(2).wait_send()

    for n in range(1, 3):
        a_copy(n).wait_send()
    p_copy().wait_send()
    for n in range(2):
        d_copy(n).wait_send()
    for r in range(rhs):
        for i in range(2):
            in_copy(r, i).wait_send()
    q_copy().wait_send()
    q_copy(True).wait_recv()
    for n in range(len(PIECES)):
        f_copy(n).wait_send()
        for i in range(2):
            y_copy(n, i).wait_send()
            y_copy(n, i, True).wait_recv()


def solution(mesh):
    def local(w, x):
        rhs, rows, cols = x.shape
        sems = []
        for shape in ((3,), (rhs, 2), (2,), (len(PIECES),), (1,), (len(PIECES), 2), (1,)):
            sems += [pltpu.SemaphoreType.DMA(shape)] * 2
        return pl.pallas_call(
            kernel,
            out_shape=pltpu.VMEM(x.shape, x.dtype),
            in_specs=[pl.BlockSpec(memory_space=pl.ANY)] * 2,
            out_specs=pl.BlockSpec(memory_space=pltpu.VMEM),
            scratch_shapes=[
                pltpu.VMEM((2, 2, rows, w.shape[1] * 2), w.dtype),
                pltpu.VMEM((rhs, 2, 2, 2, rows, cols // SIDE), x.dtype),
                pltpu.VMEM((rhs, SIDE * rows, cols // SIDE), x.dtype),
                *sems,
                pltpu.SemaphoreType.DMA((2,)),
                pltpu.SemaphoreType.REGULAR,
                pltpu.VMEM((2, MOVED, w.shape[1]), w.dtype),
                pltpu.VMEM((2, MOVED // 2, w.shape[1]), w.dtype),
                pltpu.SemaphoreType.DMA((6,)),
                pltpu.SemaphoreType.DMA((6,)),
            ],
            compiler_params=pltpu.CompilerParams(collective_id=0, has_side_effects=True, vmem_limit_bytes=52 * 1024 * 1024),
        )(w, x)

    return jax.shard_map(local, mesh=mesh, in_specs=(P(("row", "depth"), "col"), P(None, ("row", "depth"), "col")),
                         out_specs=P(None, ("row", "depth"), "col"), check_vma=False)
```

```python
import functools

import jax
import jax.numpy as jnp
from jax import lax
from jax.experimental import pallas as pl
from jax.experimental.pallas import tpu as pltpu
from jax.sharding import PartitionSpec as P

MESH = pl.DeviceIdType.MESH
SIDE = 4
PIECES = ((0, 0, 1024), (1, 0, 1024), (2, 0, 512), (2, 512, 256), (2, 768, 256))
SPLIT = 2
WIDE = 256
MOVED = 16


def kernel(w_ref, x_ref, y_ref, a_buf, x_buf, y_buf, a_send, a_recv, in_send, in_recv, d_send, d_recv, f_send, f_recv,
           p_send, p_recv, y_send, y_recv, q_send, q_recv, own_sem, ready, e_buf, g_buf, e_send, e_recv):
    z, j, row = lax.axis_index("depth"), lax.axis_index("col"), lax.axis_index("row")
    x, c = row // 2, row % 2
    rhs, rows, cols = x_ref.shape
    kcols = w_ref.shape[1]
    group = cols // SIDE

    def peer(k):
        kz, kc, kx = k // 4 % 2, k // 2 % 2, k % 2
        return x + kx * (1 - 2 * x), c + kc * (1 - 2 * c), z + kz * (1 - 2 * z)

    def device(k):
        px, pc, pz = peer(k)
        return (pz, j, px * 2 + pc)

    def in_side(k):
        px, pc, _ = peer(k)
        return pc * 2 + px

    other_y = (z, 1 - j, row)

    def remote(src, dst, send, recv, to):
        return pltpu.make_async_remote_copy(src, dst, send, recv, device_id=to, device_id_type=MESH)

    def a_block(k, jj):
        px, pc, _ = peer(k)
        return a_buf.at[pc, px, :, pl.ds(pl.multiple_of(jj * kcols, kcols), kcols)]

    def rows_of(k):
        return pl.ds(pl.multiple_of(in_side(k) * rows, rows), rows)

    def a_copy(n, receive=False):
        if n == 0:
            src, here, to = w_ref, a_block(1, j), device(1)
            there = a_block(0, j)
        elif n == 1:
            there, here = (a_buf.at[c, :, :, pl.ds(pl.multiple_of(jj * kcols, kcols), kcols)] for jj in (j, 1 - j))
            src, to = there, other_y
        else:
            there, here = a_buf.at[c], a_buf.at[1 - c]
            src, to = there, device(2)
        return remote(src, here if receive else there, a_send.at[n], a_recv.at[n], to)

    few = MOVED // 2
    last = pl.ds(rows - few, few)

    def a_over_x(op):
        low = (j == 0) & (z == 0) & (c == 1)
        high = (z == 0) & (c == 0)

        def some(cut_low, cut_high):
            at = pl.ds(MOVED * cut_low, rows - MOVED * cut_low - few * cut_high)

            def copy(receive=False):
                dst = a_block(1 if receive else 0, j).at[at, :]
                return remote(w_ref.at[at, :], dst, a_send.at[0], a_recv.at[0], device(1))

            has_low = low if cut_low else jnp.logical_not(low)
            has_high = high if cut_high else jnp.logical_not(high)
            pl.when(has_low & has_high)(lambda: op(copy))

        for cut_low in range(2):
            for cut_high in range(2):
                some(cut_low, cut_high)

    def g_copy(n):
        at = (last, slice(None))
        src, there, to = (
            (w_ref.at[at], g_buf.at[0], device(4)),
            (g_buf.at[0], g_buf.at[1], device(1)),
            (g_buf.at[1], a_block(1, j).at[at], device(4)),
        )[n]
        return remote(src, there, e_send.at[3 + n], e_recv.at[3 + n], to)

    def when_at(pz, body):
        pl.when((z == pz) & (c == 0))(body)

    def e_copy(n, receive=False):
        if n == 0:
            src, there, to = w_ref.at[pl.ds(0, MOVED), :], e_buf.at[0], other_y
        elif n == 1:
            src, there, to = e_buf.at[0], e_buf.at[1], device(1)
        else:
            src, there, to = e_buf.at[1], a_block(1, 0).at[pl.ds(0, MOVED), :], other_y
        return remote(src, there, e_send.at[n], e_recv.at[n], to)

    def when_moved(plane, body):
        pl.when((j == plane) & (z == 0) & (c == 1))(body)

    def given(piece, k):
        r, at, width = piece
        return (r, slice(None), pl.ds(pl.multiple_of(in_side(k) * group + at, WIDE), width))

    def held(piece, k):
        r, at, width = piece
        px, pc, pz = peer(k)
        return x_buf.at[r, px, pc, pz, :, pl.ds(at, width)]

    def x_copy(piece, k, send, recv, receive=False):
        return remote(x_ref.at[given(piece, k)], held(piece, k if receive else 0), send, recv, device(k))

    def in_copy(r, i, receive=False):
        return x_copy((r, 0, group), (1, 3)[i], in_send.at[r, i], in_recv.at[r, i], receive)

    def onward(piece, side, send, recv, receive):
        r, at, width = piece
        src, here = (x_buf.at[r, side, :, pz, :, pl.ds(at, width)] for pz in (z, 1 - z))
        return remote(src, here if receive else src, send, recv, device(4))

    ahead = (pl.ds(0, SPLIT), 0, group)

    def d_copy(n, receive=False):
        if n == 0:
            return x_copy(ahead, 4, d_send.at[n], d_recv.at[n], receive)
        src, here = (x_buf.at[ahead[0], x, 1 - c, pz] for pz in (z, 1 - z))
        return remote(src, here if receive else src, d_send.at[n], d_recv.at[n], device(4))

    def f_copy(n, receive=False):
        side = 1 - x if PIECES[n][0] < SPLIT else slice(None)
        return onward(PIECES[n], side, f_send.at[n], f_recv.at[n], receive)

    everything = (slice(None), 0, group)

    def p_copy(receive=False):
        return x_copy(everything, 2, p_send.at[0], p_recv.at[0], receive)

    def y_copy(n, kc, receive=False):
        k = kc * 2 + 1
        r, at, width = PIECES[n]
        src = y_buf.at[r, rows_of(k), pl.ds(at, width)]
        return remote(src, y_ref.at[given(PIECES[n], k if receive else 0)], y_send.at[n, kc], y_recv.at[n, kc], device(k))

    def q_copy(receive=False):
        there = y_ref.at[given(everything, 2 if receive else 0)]
        return remote(y_buf.at[:, rows_of(2), :], there, q_send.at[0], q_recv.at[0], device(2))

    own_a = pltpu.make_async_copy(w_ref, a_block(0, j), own_sem.at[0])
    own_x = pltpu.make_async_copy(x_ref.at[given(everything, 0)], held(everything, 0), own_sem.at[1])

    def product(k, r, at):
        xs = x_buf[r, :, :, :, :, pl.ds(at, WIDE)].reshape(-1, WIDE)
        return jnp.dot(a_buf[peer(k)[1], peer(k)[0]], xs, preferred_element_type=jnp.float32).astype(y_buf.dtype)

    def forward(n):
        r, at, _ = PIECES[n]
        if at == 0:
            for i in range(2):
                in_copy(r, i, True).wait_recv()
        f_copy(n).start()

    def multiply(n):
        r, at, width = PIECES[n]
        if n == 0:
            for m in range(2):
                d_copy(m, True).wait_recv()
        f_copy(n, True).wait_recv()
        parts = width // WIDE

        def tile(s, carry):
            t, at_s = s // parts, at + s % parts * WIDE
            kz = 1 - t // 2
            k = (t % 2 + t // 2) % 2 * 2 + kz
            at_s = pl.multiple_of(at_s, WIDE)
            y_buf[r, rows_of(k), pl.ds(at_s, WIDE)] = product(k, r, at_s)

            @pl.when(s % parts == 0)
            def _():
                for i in range(2):
                    @pl.when(t == i + 1)
                    def _():
                        y_copy(n, i).start()

            return carry

        lax.fori_loop(0, 3 * parts, tile, 0)

        def own(s, carry):
            at_s = pl.multiple_of(at + s * WIDE, WIDE)
            y_ref[r, :, pl.ds(pl.multiple_of(in_side(0) * group + at_s, WIDE), WIDE)] = product(0, r, at_s)
            return carry

        lax.fori_loop(0, parts, own, 0)

    barrier = pltpu.get_barrier_semaphore()
    pl.semaphore_signal(barrier, inc=1, device_id=device(1), device_id_type=MESH)
    beside = (device(4), other_y, device(2))
    own_x.start()
    own_a.start()

    @pl.when(x == 0)
    def _():
        for to in beside:
            pl.semaphore_signal(barrier, inc=1, device_id=to, device_id_type=MESH)
        pl.semaphore_wait(barrier, 4)
        for to in beside:
            pl.semaphore_signal(ready, inc=1, device_id=to, device_id_type=MESH)

    @pl.when(x == 1)
    def _():
        pl.semaphore_wait(barrier, 1)

    def other_links():
        when_at(0, lambda: g_copy(0).start())
        d_copy(0).start()
        p_copy().start()

    a_over_x(lambda copy: copy().start())
    pl.when(x == 0)(other_links)

    @pl.when(x == 0)
    def _():
        pl.semaphore_wait(ready, 3)
        pl.semaphore_signal(ready, inc=1, device_id=device(1), device_id_type=MESH)

    @pl.when(x == 1)
    def _():
        pl.semaphore_wait(ready, 1)
        other_links()

    when_moved(0, lambda: e_copy(0).start())

    @functools.partial(when_moved, 1)
    def _():
        e_copy(0, True).wait_recv()
        e_copy(1).start()

    @functools.partial(when_at, 1)
    def _():
        g_copy(0).wait_recv()
        g_copy(1).start()

    for r in range(rhs):
        for i in range(2):
            in_copy(r, i).start()
    own_x.wait()
    p_copy(True).wait_recv()

    @functools.partial(when_at, 1)
    def _():
        g_copy(1).wait_recv()
        g_copy(2).start()

    d_copy(1).start()
    own_a.wait()
    a_over_x(lambda copy: copy(True).wait_recv())

    @functools.partial(when_moved, 1)
    def _():
        e_copy(1, True).wait_recv()
        e_copy(2).start()

    when_moved(0, lambda: e_copy(2, True).wait_recv())
    when_at(0, lambda: g_copy(2).wait_recv())
    a_copy(1).start()
    forward(0)
    a_copy(1, True).wait_recv()
    a_copy(2).start()
    a_copy(2, True).wait_recv()
    forward(1)
    multiply(0)
    forward(2)
    multiply(1)
    forward(3)
    forward(4)
    for n in range(2, len(PIECES)):
        multiply(n)

    q_copy().start()
    a_over_x(lambda copy: copy().wait_send())
    when_at(0, lambda: g_copy(0).wait_send())
    when_at(1, lambda: g_copy(1).wait_send())
    when_at(1, lambda: g_copy(2).wait_send())
    when_moved(0, lambda: e_copy(0).wait_send())

    @functools.partial(when_moved, 1)
    def _():
        e_copy(1).wait_send()
        e_copy(2).wait_send()

    for n in range(1, 3):
        a_copy(n).wait_send()
    p_copy().wait_send()
    for n in range(2):
        d_copy(n).wait_send()
    for r in range(rhs):
        for i in range(2):
            in_copy(r, i).wait_send()
    q_copy().wait_send()
    q_copy(True).wait_recv()
    for n in range(len(PIECES)):
        f_copy(n).wait_send()
        for i in range(2):
            y_copy(n, i).wait_send()
            y_copy(n, i, True).wait_recv()


def solution(mesh):
    def local(w, x):
        rhs, rows, cols = x.shape
        sems = []
        for shape in ((3,), (rhs, 2), (2,), (len(PIECES),), (1,), (len(PIECES), 2), (1,)):
            sems += [pltpu.SemaphoreType.DMA(shape)] * 2
        return pl.pallas_call(
            kernel,
            out_shape=pltpu.VMEM(x.shape, x.dtype),
            in_specs=[pl.BlockSpec(memory_space=pl.ANY)] * 2,
            out_specs=pl.BlockSpec(memory_space=pltpu.VMEM),
            scratch_shapes=[
                pltpu.VMEM((2, 2, rows, w.shape[1] * 2), w.dtype),
                pltpu.VMEM((rhs, 2, 2, 2, rows, cols // SIDE), x.dtype),
                pltpu.VMEM((rhs, SIDE * rows, cols // SIDE), x.dtype),
                *sems,
                pltpu.SemaphoreType.DMA((2,)),
                pltpu.SemaphoreType.REGULAR,
                pltpu.VMEM((2, MOVED, w.shape[1]), w.dtype),
                pltpu.VMEM((2, MOVED // 2, w.shape[1]), w.dtype),
                pltpu.SemaphoreType.DMA((6,)),
                pltpu.SemaphoreType.DMA((6,)),
            ],
            compiler_params=pltpu.CompilerParams(collective_id=0, has_side_effects=True, vmem_limit_bytes=52 * 1024 * 1024),
        )(w, x)

    return jax.shard_map(local, mesh=mesh, in_specs=(P(("row", "depth"), "col"), P(None, ("row", "depth"), "col")),
                         out_specs=P(None, ("row", "depth"), "col"), check_vma=False)
```
